32 devices in a mesh: batch: 1 (over z), row: 4 (over y), col: 8 (over x, core).
Axes of the slice: x: 4, y: 4, z: 1, core: 2. Of those that a mesh axis runs over, the one named last changes fastest.
The devices are a block of a 4x4x8 slice.
Arguments:
- lower_tri: bfloat16 [14336, 14336], P(('batch', 'row'), 'col')
- right_side: bfloat16 [14336, 4096], P(('batch', 'row'), 'col')
- grad_out: bfloat16 [14336, 4096], P(('batch', 'row'), 'col')
Outputs:
- output 1: bfloat16 [14336, 4096], P(('batch', 'row'), 'col')
- output 2: bfloat16 [14336, 14336], P(('batch', 'row'), 'col')
All inputs are finite; a program needn't handle non-finite values.
Results may differ from the reference program's by a relative error of at most 0.001.
Values are sent between devices in bfloat16 or wider.
A program may use at most 768 MiB of HBM per device.

```python
import jax
import jax.numpy as jnp

MAT_ORDER = 14336
BLOCK_SIZE = 256
RHS_COLS = 4096
MESH_ROWS = 4
MESH_COLS = 8
ROW_BLOCKS = MAT_ORDER // (BLOCK_SIZE * MESH_ROWS)
COL_BLOCKS = MAT_ORDER // (BLOCK_SIZE * MESH_COLS)


def rows_to_global(stored):
    num_cols = stored.shape[1]
    return stored.reshape(MESH_ROWS, ROW_BLOCKS, BLOCK_SIZE, num_cols).transpose(1, 0, 2, 3).reshape(MAT_ORDER, num_cols)


def rows_to_stored(natural):
    num_cols = natural.shape[1]
    return natural.reshape(ROW_BLOCKS, MESH_ROWS, BLOCK_SIZE, num_cols).transpose(1, 0, 2, 3).reshape(MAT_ORDER, num_cols)


def cols_to_global(stored):
    num_rows = stored.shape[0]
    return stored.reshape(num_rows, MESH_COLS, COL_BLOCKS, BLOCK_SIZE).transpose(0, 2, 1, 3).reshape(num_rows, MAT_ORDER)


def cols_to_stored(natural):
    num_rows = natural.shape[0]
    return natural.reshape(num_rows, COL_BLOCKS, MESH_COLS, BLOCK_SIZE).transpose(0, 2, 1, 3).reshape(num_rows, MAT_ORDER)


def setup_inputs(seed: int = 0, part: int = 0) -> dict:
    base_key = jax.random.fold_in(jax.random.key(seed), part)
    key_lower, key_right, key_grad = jax.random.split(base_key, 3)
    lower_mat = jax.random.normal(key_lower, (MAT_ORDER, MAT_ORDER), jnp.float32) * (MAT_ORDER ** -0.5)
    lower_mat = jnp.tril(lower_mat).astype(jnp.bfloat16)
    right_mat = jax.random.normal(key_right, (MAT_ORDER, RHS_COLS), jnp.float32) * (RHS_COLS ** -0.5)
    grad_mat = jax.random.normal(key_grad, (MAT_ORDER, RHS_COLS), jnp.float32)
    return {
        "lower_tri": cols_to_stored(rows_to_stored(lower_mat)),
        "right_side": rows_to_stored(right_mat.astype(jnp.bfloat16)),
        "grad_out": rows_to_stored(grad_mat.astype(jnp.bfloat16)),
    }


def reference(lower_tri, right_side, grad_out):
    lower_mat = cols_to_global(rows_to_global(lower_tri))
    right_mat = rows_to_global(right_side)
    grad_mat = rows_to_global(grad_out)
    grad_right = jnp.dot(lower_mat.T, grad_mat, preferred_element_type=jnp.float32)
    grad_lower = jnp.tril(jnp.dot(grad_mat, right_mat.T, preferred_element_type=jnp.float32))
    return (rows_to_stored(grad_right.astype(jnp.bfloat16)), cols_to_stored(rows_to_stored(grad_lower.astype(jnp.bfloat16))))
```

```python
import functools

import jax
import jax.numpy as jnp
from jax import lax
from jax.experimental import pallas as pl
from jax.experimental.pallas import tpu as pltpu
from jax.sharding import PartitionSpec as P

BLK = 256
NSUM = 2
BF = jnp.bfloat16
F32 = jnp.float32

SLOTS = 57
DX_EVENTS = (5, 9, 13, 17, 22, 26)
LOAD_X = (0, 2, 10, 12, 18, 20, 27, 29)
SUM_X = (1, 3, 11, 13, 19, 21, 28, 30)
SUM_LAG = 4
B_X = (0, 0, 2, 5, 9, 13, 17)
B_START, B_NUM, B_DEN, B_LAG, B_CUT = 3, 3, 4, 3, 4
L_START, L_STRIDE, L_LAG, L_CUT = 3, 3, 3, 3
Y_EVENTS = (6, 12, 18, 24, 28)
T2_A, T2_B = 33, 47
T3_A, T3_NUM, T3_DEN = 31, 8, 7


def _kernel(nr, nc, l_ref, b_ref, x_ref, db_ref, dl_ref, dxg, bc, dxt, ltg, prm, prp,
            lt_in, ltv, dxv, pv, rbm, rbp, sv, dxtv, ltb, acc2, o2, dt, bv, acc3, o3, zero,
            dxs, dxr, bxs, bxr, bys, byr, dys, dyr, lys, lts, ltr, prs, prr, dbs, dbr,
            s_lin, s_dxv, s_rb, s_dxt, s_ltb, s_o2, s_dt, s_bv, s_o3, s_zero, s_own):
    rows, cols = l_ref.shape
    width = x_ref.shape[1]
    ch = 2 * BLK
    nq = rows // ch
    nb = cols // BLK
    tail = [(b, q) for b in range(NSUM, nb) for q in range(b, nq)]
    head = [(b, q) for b in range(NSUM) for q in range(b, nq)]
    nt = len(tail)
    off = {}
    for n, (b, q) in enumerate(tail + head):
        off.setdefault(b, n)
    half = rows // 2
    yrow0 = NSUM * ch
    yhalf = (rows - yrow0) // 2
    per_cut = nt // L_CUT

    z = lax.axis_index("batch")
    r = lax.axis_index("row")
    c = lax.axis_index("col")

    def dev(row, col):
        return (z, row, col)

    def remote(src, dst, ss, rs, to):
        return pltpu.make_async_remote_copy(src, dst, ss, rs, device_id=to, device_id_type=pl.DeviceIdType.MESH)

    def arrived(dst, sem):
        pltpu.make_async_copy(dst, dst, sem).wait()

    def mod(v, m):
        return lax.rem(v + 4 * m, m)

    par = lax.rem(c, 2)
    eps = 1 - 2 * par
    sib = c + eps
    far = mod(c + 4, nc)
    first = mod(c - 2 * eps, nc)
    second = mod(c + 2 * eps, nc)
    hf = par
    hs = 1 - par
    t = lax.rem(c, nr)
    sg = 1 - 2 * lax.rem(t, 2)
    d = mod((r - t) * sg, nr)
    is_root = d == 0
    qc = c // nr

    def row_of(dd):
        return mod(t + sg * dd, nr)

    def piece(o):
        vals = (0, 1, -2, 3, 2, -1, 4, 5)
        v = jnp.int32(vals[0])
        for i in range(1, 8):
            v = jnp.where(o == i, vals[i], v)
        return mod(c + eps * v, nc)

    def block_of(n, order):
        b = jnp.int32(order[0][0])
        st = jnp.int32(0)
        seen = order[0][0]
        for i, (bb, _) in enumerate(order):
            if bb != seen:
                b = jnp.where(n >= i, bb, b)
                st = jnp.where(n >= i, i, st)
                seen = bb
        return b, n - st + b

    bar = pltpu.get_barrier_semaphore()
    for k in range(1, nc):
        pl.semaphore_signal(bar, inc=1, device_id=dev(r, mod(c + k, nc)), device_id_type=pl.DeviceIdType.MESH)
    for k in range(1, nr):
        pl.semaphore_signal(bar, inc=1, device_id=dev(mod(r + k, nr), c), device_id_type=pl.DeviceIdType.MESH)
    pl.semaphore_wait(bar, nc + nr - 2)

    sends = []

    def note(cond, make, grid=None):
        sends.append((cond, make, grid))

    def bx(b, q):
        src = b_ref.at[pl.ds((2 * b + q) * BLK, BLK)]
        return remote(src, bc.at[b, c], bxs.at[b, q], bxr.at[b, c], dev(r, r + nr * q))

    def bx_start(b):
        for q in range(2):
            @pl.when(c != r + nr * q)
            def _():
                bx(b, q).start()

    for b in range(nb):
        for q in range(2):
            note(c != r + nr * q, functools.partial(bx, b, q))

    def dx_own(h, to, i):
        src = x_ref.at[pl.ds(h * half, half)]
        return remote(src, dxg.at[c, pl.ds(h * half, half)], dxs.at[i], dxr.at[c, h], dev(r, to))

    def dx_fwd(p, h, to, i):
        ref = dxg.at[p, pl.ds(h * half, half)]
        return remote(ref, ref, dxs.at[i], dxr.at[p, h], dev(r, to))

    def dx_wait(p, h):
        arrived(dxg.at[p, pl.ds(h * half, half)], dxr.at[p, h])

    own_list = [functools.partial(dx_own, hf, second, 0), functools.partial(dx_own, hs, first, 2),
                functools.partial(dx_own, hf, sib, 4), functools.partial(dx_own, hs, sib, 5),
                functools.partial(dx_own, hs, second, 1), functools.partial(dx_own, hf, first, 3)]
    ev = [(first, hf, [functools.partial(dx_fwd, first, hf, second, 6), functools.partial(dx_fwd, first, hf, sib, 7)]),
          (first, hs, [functools.partial(dx_fwd, first, hs, sib, 8)]),
          (second, hs, [functools.partial(dx_fwd, second, hs, first, 9), functools.partial(dx_fwd, second, hs, sib, 10)]),
          (second, hf, [functools.partial(dx_fwd, second, hf, sib, 11)]),
          (far, hf, [functools.partial(dx_fwd, far, hf, sib, 12)]),
          (far, hs, [functools.partial(dx_fwd, far, hs, sib, 13)])]
    for m in own_list:
        note(None, m)
    for _, _, ms in ev:
        for m in ms:
            note(None, m)

    up = mod(r + 1, nr)
    down = mod(r + nr - 1, nr)
    opp = mod(r + 2, nr)

    def dy_own(h, to, i):
        src = x_ref.at[pl.ds(yrow0 + h * yhalf, yhalf)]
        return remote(src, dxt.at[r, pl.ds(h * yhalf, yhalf)], dys.at[i], dyr.at[r, h], dev(to, c))

    def dy_fwd(p, h, to, i):
        ref = dxt.at[p, pl.ds(h * yhalf, yhalf)]
        return remote(ref, ref, dys.at[i], dyr.at[p, h], dev(to, c))

    def dy_wait(p, h):
        arrived(dxt.at[p, pl.ds(h * yhalf, yhalf)], dyr.at[p, h])

    dy_list = [functools.partial(dy_own, 0, up, 0), functools.partial(dy_own, 1, down, 1),
               functools.partial(dy_own, 1, up, 2), functools.partial(dy_own, 0, down, 3),
               functools.partial(dy_fwd, down, 0, up, 4), functools.partial(dy_fwd, up, 1, down, 5)]
    for m in dy_list:
        note(None, m)

    bx_start(0)
    bx_start(1)
    for m in own_list:
        m().start()
    dy_list[0]().start()
    dy_list[1]().start()

    def load_x(o, slot):
        return pltpu.make_async_copy(x_ref, dxv.at[slot], s_dxv.at[slot])

    load_x(0, 0).start()

    def own_b(b):
        return pltpu.make_async_copy(b_ref.at[pl.ds((2 * b + qc) * BLK, BLK)], sv.at[b, pl.ds(0, BLK)], s_own.at[b])

    def own_b_out(b):
        return pltpu.make_async_copy(sv.at[b, pl.ds(0, BLK)], bc.at[b, c], bxr.at[b, c])

    @pl.when(is_root)
    def _():
        for b in range(nb):
            own_b(b).start()

    zero[...] = jnp.zeros_like(zero)
    zeros = [(b, q) for b in range(nb) for q in range(b)]

    def zero_copy(i):
        b, q = zeros[i]
        return pltpu.make_async_copy(zero, dl_ref.at[pl.ds(q * ch, ch), pl.ds(b * BLK, BLK)], s_zero.at[i])

    for i in range(len(zeros)):
        zero_copy(i).start()

    order = tail + head
    ntot = len(order)

    def lin(n):
        b, q = block_of(n, order)
        src = l_ref.at[pl.ds(pl.multiple_of(q * ch, ch), ch), pl.ds(pl.multiple_of(b * BLK, BLK), BLK)]
        return pltpu.make_async_copy(src, lt_in.at[lax.rem(n, 2)], s_lin.at[lax.rem(n, 2)])

    def ly(i):
        return remote(ltv.at[pl.ds(i * per_cut, per_cut)], ltg.at[qc, r, pl.ds(i * per_cut, per_cut)],
                      lys.at[i], ltr.at[qc, r, i], dev(t, c))

    def l_own(i):
        return pltpu.make_async_copy(ltv.at[pl.ds(i * per_cut, per_cut)], ltg.at[qc, r, pl.ds(i * per_cut, per_cut)],
                                     ltr.at[qc, r, i])

    for i in range(L_CUT):
        note(d != 0, functools.partial(ly, i))

    lin(0).start()

    @pl.loop(0, ntot)
    def _(n):
        lin(n).wait()

        @pl.when(n + 1 < ntot)
        def _():
            lin(n + 1).start()

        ltv[n] = lt_in[lax.rem(n, 2)].T
        for i in range(L_CUT):
            @pl.when(n == (i + 1) * per_cut - 1)
            def _():
                @pl.when(is_root)
                def _():
                    l_own(i).start()

                @pl.when(d != 0)
                def _():
                    ly(i).start()

    @pl.when(is_root)
    def _():
        for b in range(nb):
            own_b(b).wait()
        for b in range(nb):
            own_b_out(b).start()

    on_ring = par == lax.rem(r, 2)

    def l_send(q, e, w, to):
        rr = mod(r + lax.rem(e, nr), nr)
        i = e // nr
        ref = ltg.at[q, rr, pl.ds(i * per_cut, per_cut)]
        return remote(ref, ref, lts.at[e, q, w], ltr.at[q, rr, i], dev(r, to))

    def l_wait(q, e):
        rr = mod(r + lax.rem(e, nr), nr)
        i = e // nr
        arrived(ltg.at[q, rr, pl.ds(i * per_cut, per_cut)], ltr.at[q, rr, i])

    right = mod(c + 2, nc)
    left = mod(c - 2, nc)
    ne = nr * L_CUT

    def l_fwd(q, e):
        side = lax.rem(e, nr) // 2
        from_left = c == mod(r + nr * q + 2, nc)
        cond = jnp.logical_and(jnp.logical_and(on_ring, jnp.logical_not(is_root)), from_left == (side == 0))
        return cond, l_send(q, e, 0, jnp.where(from_left, right, left))

    def l_stage0(e):
        l_wait(qc, e)
        l_send(qc, e, 0, right).start()
        l_send(qc, e, 1, left).start()
        l_send(qc, e, 2, sib).start()

    def l_stage1(e):
        for q in range(2):
            l_wait(q, e)
            cond, cp = l_fwd(q, e)

            @pl.when(cond)
            def _():
                cp.start()
            l_send(q, e, 2, sib).start()

    def l_stage2(e):
        l_wait(1 - qc, e)
        l_send(1 - qc, e, 2, sib).start()

    def l_stage3(e):
        for q in range(2):
            l_wait(q, e)

    bh = BLK // B_CUT
    nv = nb * B_CUT

    def b_ref_of(v, lo, hi):
        return bc.at[v // B_CUT, pl.ds(lo, hi - lo), pl.ds(lax.rem(v, B_CUT) * bh, bh)]

    def b_send(v, lo, hi, ss, rs, dd):
        ref = b_ref_of(v, lo, hi)
        return remote(ref, ref, bys.at[v, ss], byr.at[v, rs], dev(row_of(dd), c))

    def b_wait(v, lo, hi, rs):
        arrived(b_ref_of(v, lo, hi), byr.at[v, rs])

    ja, jc = 3, 6
    b_moves = [(0, lambda v: b_send(v, 0, nc, 0, 0, 3)), (0, lambda v: b_send(v, ja, nc, 1, 0, 1)),
               (3, lambda v: b_send(v, 0, jc, 0, 0, 2)), (1, lambda v: b_send(v, jc, nc, 0, 1, 2)),
               (2, lambda v: b_send(v, 0, ja, 0, 1, 1))]

    def b_active(s):
        def count(x):
            return jnp.clip((x * B_NUM) // B_DEN + 1, 0, nv)
        lo = jnp.where(s > 0, count(s - 1), 0)
        lo = jnp.where(s <= 0, 0, lo)
        hi = jnp.where(s >= 0, count(s), 0)
        return hi > lo, lo

    mrow = ch // 4
    part_rows = ((mrow, ch - mrow), (0, mrow))

    def sum_send(o, part):
        lo, n = part_rows[part]
        to = row_of(mod(d - 1, nr)) if part == 0 else row_of(mod(d + 1, nr))
        dst = (prm if part == 0 else prp).at[o]
        return remote(pv.at[o, pl.ds(lo, n)], dst, prs.at[o, part], prr.at[o, part], dev(to, c))

    def sum_step(o, part, depth):
        lo, n = part_rows[part]
        land = (prm if part == 0 else prp).at[o]
        buf = rbm if part == 0 else rbp

        @pl.when(depth > 0)
        def _():
            arrived(land, prr.at[o, part])
            cp = pltpu.make_async_copy(land, buf, s_rb.at[part])
            cp.start()
            cp.wait()

            @pl.loop(0, n // 64)
            def _(i):
                pv[o, pl.ds(lo + i * 64, 64)] = pv[o, pl.ds(lo + i * 64, 64)] + buf[pl.ds(i * 64, 64)]

        @pl.when(jnp.logical_not(is_root))
        def _():
            sum_send(o, part).start()

    def out_send(o, b, to):
        dst = db_ref.at[pl.ds((2 * b + qc) * BLK, BLK)]
        return remote(sv.at[o, pl.ds(b * BLK, BLK)], dst, dbs.at[o, b], dbr.at[2 * b + qc], dev(r, to))

    def out_local(o, b):
        dst = db_ref.at[pl.ds((2 * b + qc) * BLK, BLK)]
        return pltpu.make_async_copy(sv.at[o, pl.ds(b * BLK, BLK)], dst, dbr.at[2 * b + qc])

    def finish(o):
        @pl.loop(0, ch // 64)
        def _(i):
            sv[o, pl.ds(i * 64, 64)] = pv[o, pl.ds(i * 64, 64)].astype(BF)

        for b in range(NSUM):
            @pl.when(o == 0)
            def _():
                out_local(o, b).start()

            @pl.when(o != 0)
            def _():
                out_send(o, b, piece(o)).start()

    def sum_index(s):
        act = s == SUM_X[0]
        o = jnp.int32(0)
        for i in range(1, 8):
            hit = s == SUM_X[i]
            act = jnp.logical_or(act, hit)
            o = jnp.where(hit, i, o)
        return act, o

    def partial(o):
        slot = lax.rem(o, 2)
        for b in range(NSUM):
            @pl.loop(b, nq)
            def _(q):
                v = jnp.dot(ltv[off[b] + q - b], dxv[slot, pl.ds(pl.multiple_of(q * ch, ch), ch)], preferred_element_type=F32)

                @pl.when(q == b)
                def _():
                    pv[o, pl.ds(b * BLK, BLK)] = v

                @pl.when(q != b)
                def _():
                    pv[o, pl.ds(b * BLK, BLK)] = pv[o, pl.ds(b * BLK, BLK)] + v

    def t2_of(w):
        g = w // nr
        b = NSUM + g // 2
        st = jnp.int32(off[NSUM])
        for bb in range(NSUM + 1, nb):
            st = jnp.where(b == bb, off[bb], st)
        return b, lax.rem(g, 2), lax.rem(w, nr), st

    n2 = (nb - NSUM) * 2 * nr

    def t2_load(w, i):
        b, q, rr, st = t2_of(w)
        k = lax.rem(w, 2)
        return pltpu.make_async_copy(ltg.at[q, rr, st + i], ltb.at[k, i], s_ltb.at[k, i])

    def t2_start(w):
        b = t2_of(w)[0]

        @pl.loop(0, nq - b)
        def _(i):
            t2_load(w, i).start()

    def t2_out(g):
        b, q = NSUM + g // 2, lax.rem(g, 2)
        k = lax.rem(g, 2)
        return pltpu.make_async_copy(o2.at[k], db_ref.at[pl.ds((2 * b + q) * BLK, BLK)], s_o2.at[k])

    def t2_item(w):
        b, q, rr, _ = t2_of(w)
        k = lax.rem(w, 2)
        g = w // nr

        @pl.loop(0, nq - b)
        def _(i):
            t2_load(w, i).wait()

        @pl.when(w + 1 < n2)
        def _():
            t2_start(w + 1)

        @pl.loop(0, nq - b)
        def _(i):
            v = jnp.dot(ltb[k, i], dxtv[rr, pl.ds(pl.multiple_of((b + i - NSUM) * ch, ch), ch)], preferred_element_type=F32)
            fresh = jnp.logical_and(rr == 0, i == 0)

            @pl.when(fresh)
            def _():
                acc2[...] = v

            @pl.when(jnp.logical_not(fresh))
            def _():
                acc2[...] = acc2[...] + v

        @pl.when(rr == nr - 1)
        def _():
            @pl.when(g >= 2)
            def _():
                t2_out(g - 2).wait()
            o2[lax.rem(g, 2)] = acc2[...].astype(BF)
            t2_out(g).start()

    t3_order = [(b, q) for b in range(nb) for q in range(b, nq)]
    n3 = len(t3_order)
    t3_last = [max(n for n, (bb, _) in enumerate(t3_order) if bb == b) for b in range(nb)]

    def t3_load(n, o):
        b, q = block_of(n, t3_order)
        k = lax.rem(n, 2)
        rws = pl.ds(pl.multiple_of(q * ch, ch), ch)
        src = x_ref.at[rws] if o == 0 else dxg.at[mod(c + o, nc), rws]
        return pltpu.make_async_copy(src, dt.at[k, o], s_dt.at[k, o])

    def bv_load(b):
        return pltpu.make_async_copy(bc.at[b], bv.at[lax.rem(b, 2)], s_bv.at[lax.rem(b, 2)])

    def t3_out(n):
        b, q = block_of(n, t3_order)
        k = lax.rem(n, 2)
        dst = dl_ref.at[pl.ds(pl.multiple_of(q * ch, ch), ch), pl.ds(pl.multiple_of(b * BLK, BLK), BLK)]
        return pltpu.make_async_copy(o3.at[k], dst, s_o3.at[k])

    def t3_item(n):
        b, q = block_of(n, t3_order)
        k = lax.rem(n, 2)
        for o in range(nc):
            t3_load(n, o).wait()

        @pl.when(n + 1 < n3)
        def _():
            for o in range(nc):
                t3_load(n + 1, o).start()

        @pl.when(q == b)
        def _():
            bv_load(b).wait()

        @pl.loop(0, nc)
        def _(o):
            v = lax.dot_general(dt[k, o], bv[lax.rem(b, 2), mod(c + o, nc)], (((1,), (1,)), ((), ())), preferred_element_type=F32)

            @pl.when(o == 0)
            def _():
                acc3[...] = v

            @pl.when(o != 0)
            def _():
                acc3[...] = acc3[...] + v

        @pl.when(n >= 2)
        def _():
            t3_out(n - 2).wait()

        for i in range(ch // 128):
            pos = lax.broadcasted_iota(jnp.int32, (128, BLK), 0) + i * 128
            kpos = lax.broadcasted_iota(jnp.int32, (128, BLK), 1)
            rg = ((2 * q + i * 128 // BLK) * nr + r) * BLK + pos % BLK
            cg = (b * nc + c) * BLK + kpos
            o3[k, pl.ds(i * 128, 128)] = jnp.where(rg >= cg, acc3[pl.ds(i * 128, 128)], 0.0).astype(BF)
        t3_out(n).start()
        for b2 in range(nb - 2):
            @pl.when(n == t3_last[b2])
            def _():
                bv_load(b2 + 2).start()

    def t3_count(s):
        return jnp.where(s < T3_A, 0, jnp.clip(((s - T3_A) * T3_NUM) // T3_DEN + 1, 0, n3))

    def t2_count(s):
        first_part = 4 * 2 * 2
        return jnp.clip(s - T2_A + 1, 0, first_part) + jnp.clip((s - T2_B + 1) * 4, 0, n2 - first_part)

    def b_slot(v):
        return B_START + min(x for x in range(200) if (x * B_NUM) // B_DEN + 1 > v)

    def t3_slot(n):
        return T3_A + min(x for x in range(200) if (x * T3_NUM) // T3_DEN + 1 > n)

    for b in range(nb):
        ready = b_slot(B_CUT * b + B_CUT - 1) + 3 * B_LAG
        n0 = 0 if b < 2 else t3_last[b - 2]
        assert t3_slot(n0) >= ready, (b, ready, t3_slot(n0))
    assert T3_A > LOAD_X[7] and T3_A - 1 >= LOAD_X[7]
    assert L_START + L_STRIDE * (2 * nr - 1) + 3 * L_LAG < T2_A + 7 and L_START + L_STRIDE * (ne - 1) + 3 * L_LAG < T2_B
    assert t3_slot(n3 - 1) < SLOTS and T2_B + 6 <= SLOTS and SUM_X[7] + 3 * SUM_LAG < SLOTS

    @pl.loop(0, SLOTS)
    def _(s):
        for i, (p, h, ms) in enumerate(ev):
            @pl.when(s == DX_EVENTS[i])
            def _():
                dx_wait(p, h)
                for m in ms:
                    m().start()

        def l_at(stage, fn, cond):
            x = s - L_START - L_LAG * stage
            act = jnp.logical_and(jnp.logical_and(x >= 0, x < ne * L_STRIDE), lax.rem(jnp.maximum(x, 0), L_STRIDE) == 0)

            @pl.when(jnp.logical_and(act, cond))
            def _():
                fn(x // L_STRIDE)

        l_at(0, l_stage0, is_root)
        l_at(1, l_stage1, jnp.logical_and(on_ring, jnp.logical_not(is_root)))
        l_at(2, l_stage2, is_root)
        l_at(3, l_stage3, jnp.logical_not(on_ring))

        act, v = b_active(s - B_START)

        @pl.when(jnp.logical_and(act, is_root))
        def _():
            @pl.when(lax.rem(v, B_CUT) == 0)
            def _():
                @pl.loop(0, nc)
                def _(j):
                    arrived(bc.at[v // B_CUT, j], bxr.at[v // B_CUT, j])
            b_moves[0][1](v).start()
            b_moves[1][1](v).start()

        act1, v1 = b_active(s - B_START - B_LAG)

        @pl.when(jnp.logical_and(act1, d == 3))
        def _():
            b_wait(v1, 0, nc, 0)
            b_moves[2][1](v1).start()

        @pl.when(jnp.logical_and(act1, d == 1))
        def _():
            b_wait(v1, ja, nc, 0)
            b_moves[3][1](v1).start()

        act2, v2 = b_active(s - B_START - 2 * B_LAG)

        @pl.when(jnp.logical_and(act2, d == 2))
        def _():
            b_wait(v2, 0, jc, 0)
            b_moves[4][1](v2).start()
            b_wait(v2, jc, nc, 1)

        act3, v3 = b_active(s - B_START - 3 * B_LAG)

        @pl.when(jnp.logical_and(act3, d == 1))
        def _():
            b_wait(v3, 0, ja, 1)

        for b in range(2, nb):
            @pl.when(s == B_X[b])
            def _():
                bx_start(b)

        @pl.when(s == Y_EVENTS[0])
        def _():
            dy_list[2]().start()
            dy_list[3]().start()

        @pl.when(s == Y_EVENTS[1])
        def _():
            dy_wait(down, 0)
            dy_list[4]().start()
            dy_wait(up, 1)
            dy_list[5]().start()

        @pl.when(s == Y_EVENTS[2])
        def _():
            dy_wait(down, 1)
            dy_wait(up, 0)

        @pl.when(s == Y_EVENTS[3])
        def _():
            dy_wait(opp, 0)
            dy_wait(opp, 1)

        @pl.when(s == Y_EVENTS[4])
        def _():
            pltpu.make_async_copy(x_ref.at[pl.ds(yrow0, 2 * yhalf)], dxtv.at[r], s_dxt.at[0]).start()
            for i in range(1, nr):
                rr = mod(r + i, nr)
                pltpu.make_async_copy(dxt.at[rr], dxtv.at[rr], s_dxt.at[i]).start()

        for part, depth in ((0, 3 - d), (1, mod(d - 1, nr))):
            sact, o = sum_index(s - SUM_LAG * depth)

            @pl.when(jnp.logical_and(sact, depth > 0))
            def _():
                sum_step(o, part, depth)

        fact, fo = sum_index(s - SUM_LAG * 3)

        @pl.when(jnp.logical_and(fact, is_root))
        def _():
            finish(fo)

        for o in range(1, 8):
            @pl.when(s == LOAD_X[o])
            def _():
                p = piece(o)
                if o % 2 == 1:
                    dx_wait(p, 0)
                    dx_wait(p, 1)
                pltpu.make_async_copy(dxg.at[p], dxv.at[o % 2], s_dxv.at[o % 2]).start()

        pact, po = sum_index(s)

        @pl.when(pact)
        def _():
            load_x(0, lax.rem(po, 2)).wait()
            partial(po)
            for part, depth in ((0, 3 - d), (1, mod(d - 1, nr))):
                @pl.when(depth == 0)
                def _():
                    sum_send(po, part).start()

        @pl.when(s == T2_A - 1)
        def _():
            t2_start(0)
            for i in range(nr):
                pltpu.make_async_copy(x_ref.at[pl.ds(yrow0, 2 * yhalf)], dxtv.at[r], s_dxt.at[i]).wait()

        @pl.when(s == T3_A - 1)
        def _():
            bv_load(0).start()
            bv_load(1).start()
            for o in range(nc):
                t3_load(0, o).start()

        @pl.loop(t2_count(s - 1), t2_count(s))
        def _(w):
            t2_item(w)

        @pl.loop(t3_count(s - 1), t3_count(s))
        def _(n):
            t3_item(n)

    for g in (n2 // nr - 2, n2 // nr - 1):
        t2_out(g).wait()
    for n in (n3 - 2, n3 - 1):
        t3_out(n).wait()
    for i in range(len(zeros)):
        zero_copy(i).wait()
    for i in range(2 * NSUM):
        arrived(db_ref.at[pl.ds(i * BLK, BLK)], dbr.at[i])

    for cond, make, _ in sends:
        if cond is None:
            make().wait_send()
        else:
            @pl.when(cond)
            def _():
                make().wait_send()

    @pl.loop(0, nv)
    def _(v):
        for dd, make in b_moves:
            @pl.when(d == dd)
            def _():
                make(v).wait_send()

    @pl.loop(0, ne)
    def _(e):
        @pl.when(is_root)
        def _():
            l_send(qc, e, 0, right).wait_send()
            l_send(qc, e, 1, left).wait_send()
            l_send(qc, e, 2, sib).wait_send()
            l_send(1 - qc, e, 2, sib).wait_send()

        @pl.when(jnp.logical_and(on_ring, jnp.logical_not(is_root)))
        def _():
            for q in range(2):
                cond, cp = l_fwd(q, e)

                @pl.when(cond)
                def _():
                    cp.wait_send()
                l_send(q, e, 2, sib).wait_send()

    @pl.loop(0, 8)
    def _(o):
        @pl.when(jnp.logical_not(is_root))
        def _():
            for part in range(2):
                sum_send(o, part).wait_send()

        @pl.when(jnp.logical_and(is_root, o != 0))
        def _():
            for b in range(NSUM):
                out_send(o, b, piece(o)).wait_send()


def solution(mesh):
    nr = mesh.shape["row"]
    nc = mesh.shape["col"]
    spec = P(("batch", "row"), "col")

    def per_device(lower_tri, right_side, grad_out):
        rows, cols = lower_tri.shape
        width = right_side.shape[1]
        ch = 2 * BLK
        nq, nb = rows // ch, cols // BLK
        nt = sum(nq - b for b in range(NSUM, nb))
        ntot = sum(nq - b for b in range(nb))
        yrows = rows - NSUM * ch
        nzero = nb * (nb - 1) // 2
        sd = jax.ShapeDtypeStruct
        outs = (sd((rows, width), BF), sd((rows, cols), BF), sd((nc, rows, width), BF), sd((nb, nc, BLK, width), BF),
                sd((nr, yrows, width), BF), sd((2, nr, nt, BLK, ch), BF),
                sd((8, ch - ch // 4, width), F32), sd((8, ch // 4, width), F32))
        vm = pltpu.VMEM
        dma = pltpu.SemaphoreType.DMA
        scratch = [vm((2, ch, BLK), BF), vm((ntot, BLK, ch), BF), vm((2, rows, width), BF), vm((8, ch, width), F32),
                   vm((ch - ch // 4, width), F32), vm((ch // 4, width), F32), vm((8, ch, width), BF),
                   vm((nr, yrows, width), BF), vm((2, nq - NSUM, BLK, ch), BF), vm((BLK, width), F32), vm((2, BLK, width), BF),
                   vm((2, nc, ch, width), BF), vm((2, nc, BLK, width), BF), vm((ch, BLK), F32), vm((2, ch, BLK), BF),
                   vm((ch, BLK), BF),
                   dma((14,)), dma((nc, 2)), dma((nb, 2)), dma((nb, nc)), dma((nb * B_CUT, 2)), dma((nb * B_CUT, 2)),
                   dma((6,)), dma((nr, 2)), dma((L_CUT,)), dma((nr * L_CUT, 2, 3)), dma((2, nr, L_CUT)),
                   dma((8, 2)), dma((8, 2)), dma((8, NSUM)), dma((2 * NSUM,)),
                   dma((2,)), dma((2,)), dma((2,)), dma((nr,)), dma((2, nq - NSUM)), dma((2,)), dma((2, nc)), dma((2,)),
                   dma((2,)), dma((nzero,)), dma((nb,))]
        res = pl.pallas_call(
            functools.partial(_kernel, nr, nc),
            out_shape=outs,
            in_specs=[pl.BlockSpec(memory_space=pl.ANY)] * 3,
            out_specs=tuple(pl.BlockSpec(memory_space=pl.ANY) for _ in outs),
            scratch_shapes=scratch,
            compiler_params=pltpu.CompilerParams(collective_id=0, has_side_effects=True, vmem_limit_bytes=67043328),
            name="tri_backward",
        )(lower_tri, right_side, grad_out)
        return res[0], res[1]

    return jax.shard_map(per_device, mesh=mesh, in_specs=(spec, spec, spec), out_specs=(spec, spec), check_vma=False)
```

```python
import functools

import jax
import jax.numpy as jnp
from jax import lax
from jax.experimental import pallas as pl
from jax.experimental.pallas import tpu as pltpu
from jax.sharding import PartitionSpec as P

BLK = 256
NSUM = 3
BF = jnp.bfloat16
F32 = jnp.float32

B_CUT = 4
L_CUT = 3
L_BUF = 4
DX_SEND = 20
DX_EVENTS = (28, 38, 42, 52, 61, 82)
SUM_X = (7, 9, 43, 47, 55, 57, 88, 97)
SUM_LINES = ((38, 50, 4), (73, 33, 4), (74, 40, 4))
BX_LINE = (9, 37, 4)
B_LINES = ((24, 16, 4), (40, 14, 4), (90, 8, 4), (99, 7, 4))
L_LINES = ((49, 6, 4), (84, 14, 4), (91, 13, 4), (95, 13, 4))
Y_EVENTS = (10, 15, 12, 55, 55, 65, 72)
T2_A = 125
T3_A = 98
PER_SLOT = 2
JA, JC, SUM_UP = 3, 4, 64


def _line(line, n):
    first, num, den = line
    return tuple(first + i * num // den for i in range(n))


def _kernel(nr, nc, l_ref, b_ref, x_ref, db_ref, dl_ref, dxg, bc, dxt, ltg, prm, prp,
            lt_in, ltv, lth, dxv, pv, rbm, rbp, sv, dxtv, ltb, acc2, o2, dt, bv, acc3, o3,
            dxs, dxr, bxs, bxr, bys, byr, dys, dyr, lys, lts, ltr, prs, prr, dbs, dbr,
            s_ltz, s_lin, s_dxv, s_rb, s_dxt, s_ltb, s_o2, s_dt, s_bv, s_o3, s_zero, s_own):
    rows, cols = l_ref.shape
    width = x_ref.shape[1]
    ch = 2 * BLK
    nq = rows // ch
    nb = cols // BLK
    tail = [(b, b) for b in range(NSUM, nb)] + [(b, q) for b in range(NSUM, nb) for q in range(b + 1, nq)]
    ndiag = nb - NSUM
    head = [(b, q) for b in range(NSUM) for q in range(b, nq)]
    nt = len(tail)
    off = {}
    for n, (b, q) in enumerate(tail + head):
        off.setdefault(b, n)
    half = rows // 2
    yrow0 = NSUM * ch
    yhalf = (rows - yrow0) // 2
    cuts = [n for n in range(nt) if n in (0, ndiag) or tail[n - 1][0] != tail[n][0] and n > ndiag][:L_CUT] + [nt]

    nv = nb * B_CUT
    ne = nr * L_CUT
    load_x_at = tuple(max(x - 1, 0) for x in SUM_X)
    sum_at = tuple(_line(x, nc) for x in SUM_LINES)
    bx_at = _line(BX_LINE, nb)
    b_slot = tuple(_line(x, nv) for x in B_LINES)
    l_slot = tuple(_line(x, ne) for x in L_LINES)

    z = lax.axis_index("batch")
    r = lax.axis_index("row")
    c = lax.axis_index("col")

    def dev(row, col):
        return (z, row, col)

    def remote(src, dst, ss, rs, to):
        return pltpu.make_async_remote_copy(src, dst, ss, rs, device_id=to, device_id_type=pl.DeviceIdType.MESH)

    def arrived(dst, sem):
        pltpu.make_async_copy(dst, dst, sem).wait()

    def mod(v, m):
        return lax.rem(v + 4 * m, m)

    par = lax.rem(c, 2)
    eps = 1 - 2 * par
    sib = c + eps
    far = mod(c + 4, nc)
    first = mod(c - 2 * eps, nc)
    second = mod(c + 2 * eps, nc)
    hf = par
    hs = 1 - par
    t = lax.rem(c, nr)
    sg = 1 - 2 * lax.rem(t, 2)
    d = mod((r - t) * sg, nr)
    is_root = d == 0
    qc = c // nr

    def row_of(dd):
        return mod(t + sg * dd, nr)

    def piece(o):
        vals = (0, 1, -2, 3, 2, -1, 4, 5)
        v = jnp.int32(vals[0])
        for i in range(1, 8):
            v = jnp.where(o == i, vals[i], v)
        return mod(c + eps * v, nc)

    def table(n, vals):
        v = jnp.int32(vals[0])
        for i in range(1, len(vals)):
            if vals[i] != vals[i - 1]:
                v = jnp.where(n >= i, vals[i], v)
        return v

    def block_of(n, order):
        return table(n, [b for b, _ in order]), table(n, [q for _, q in order])

    bar = pltpu.get_barrier_semaphore()
    for k in range(1, nc):
        pl.semaphore_signal(bar, inc=1, device_id=dev(r, mod(c + k, nc)), device_id_type=pl.DeviceIdType.MESH)
    for k in range(1, nr):
        pl.semaphore_signal(bar, inc=1, device_id=dev(mod(r + k, nr), c), device_id_type=pl.DeviceIdType.MESH)
    pl.semaphore_wait(bar, nc + nr - 2)

    sends = []

    def note(cond, make, grid=None):
        sends.append((cond, make, grid))

    def bx(b, q):
        src = b_ref.at[pl.ds((2 * b + q) * BLK, BLK)]
        return remote(src, bc.at[b, c], bxs.at[b, q], bxr.at[b, c], dev(r, r + nr * q))

    def bx_start(b):
        for q in range(2):
            @pl.when(c != r + nr * q)
            def _():
                bx(b, q).start()

    for b in range(nb):
        for q in range(2):
            note(c != r + nr * q, functools.partial(bx, b, q))

    def dx_own(h, to, i):
        src = x_ref.at[pl.ds(h * half, half)]
        return remote(src, dxg.at[c, pl.ds(h * half, half)], dxs.at[i], dxr.at[c, h], dev(r, to))

    def dx_fwd(p, h, to, i):
        ref = dxg.at[p, pl.ds(h * half, half)]
        return remote(ref, ref, dxs.at[i], dxr.at[p, h], dev(r, to))

    def dx_wait(p, h):
        arrived(dxg.at[p, pl.ds(h * half, half)], dxr.at[p, h])

    own_list = [functools.partial(dx_own, hf, second, 0), functools.partial(dx_own, hf, sib, 4),
                functools.partial(dx_own, hs, second, 1), functools.partial(dx_own, hs, sib, 5),
                functools.partial(dx_own, hs, first, 2), functools.partial(dx_own, hf, first, 3)]
    ev = [(first, hf, [functools.partial(dx_fwd, first, hf, second, 6), functools.partial(dx_fwd, first, hf, sib, 7)]),
          (first, hs, [functools.partial(dx_fwd, first, hs, sib, 8)]),
          (second, hs, [functools.partial(dx_fwd, second, hs, first, 9), functools.partial(dx_fwd, second, hs, sib, 10)]),
          (second, hf, [functools.partial(dx_fwd, second, hf, sib, 11)]),
          (far, hf, [functools.partial(dx_fwd, far, hf, sib, 12)]),
          (far, hs, [functools.partial(dx_fwd, far, hs, sib, 13)])]
    for m in own_list:
        note(None, m)
    for _, _, ms in ev:
        for m in ms:
            note(None, m)

    up = mod(r + 1, nr)
    down = mod(r + nr - 1, nr)
    opp = mod(r + 2, nr)

    def dy_own(h, to, i):
        src = x_ref.at[pl.ds(yrow0 + h * yhalf, yhalf)]
        return remote(src, dxt.at[r, pl.ds(h * yhalf, yhalf)], dys.at[i], dyr.at[r, h], dev(to, c))

    def dy_fwd(p, h, to, i):
        ref = dxt.at[p, pl.ds(h * yhalf, yhalf)]
        return remote(ref, ref, dys.at[i], dyr.at[p, h], dev(to, c))

    def dy_wait(p, h):
        arrived(dxt.at[p, pl.ds(h * yhalf, yhalf)], dyr.at[p, h])

    dy_list = [functools.partial(dy_own, 0, up, 0), functools.partial(dy_own, 1, down, 1),
               functools.partial(dy_own, 1, up, 2), functools.partial(dy_own, 0, down, 3),
               functools.partial(dy_fwd, down, 0, up, 4), functools.partial(dy_fwd, up, 1, down, 5)]
    for m in dy_list:
        note(None, m)

    own_list[0]().start()
    own_list[1]().start()
    bx_start(0)
    own_list[2]().start()
    own_list[3]().start()
    dy_list[0]().start()
    dy_list[1]().start()

    def load_x(o, slot):
        return pltpu.make_async_copy(x_ref, dxv.at[slot], s_dxv.at[slot])

    load_x(0, 0).start()

    def own_b(b):
        return pltpu.make_async_copy(b_ref.at[pl.ds((2 * b + qc) * BLK, BLK)], sv.at[b, pl.ds(0, BLK)], s_own.at[b])

    def own_b_out(b):
        return pltpu.make_async_copy(sv.at[b, pl.ds(0, BLK)], bc.at[b, c], bxr.at[b, c])

    @pl.when(is_root)
    def _():
        for b in range(nb):
            own_b(b).start()

    zeros = [(b, q) for b in range(nb) for q in range(b)]

    def zero_copy(i):
        b, q = zeros[i]
        return pltpu.make_async_copy(lt_in.at[0], dl_ref.at[pl.ds(q * ch, ch), pl.ds(b * BLK, BLK)], s_zero.at[i])

    order = tail + head
    ntot = len(order)

    def lin(n):
        b, q = block_of(n, order)
        src = l_ref.at[pl.ds(pl.multiple_of(q * ch, ch), ch), pl.ds(pl.multiple_of(b * BLK, BLK), BLK)]
        return pltpu.make_async_copy(src, lt_in.at[lax.rem(n, L_BUF)], s_lin.at[lax.rem(n, L_BUF)])

    def part_of(ref, i, full):
        n = cuts[i + 1] - cuts[i]
        return ref.at[pl.ds(cuts[i], n)] if full else ref.at[pl.ds(cuts[i], n), :, pl.ds(BLK, BLK)]

    def level(home, src_row, q, i):
        return jnp.where(src_row >= home, 2, 1) - q if i == 0 else jnp.int32(2)

    def by_level(i, lvl, fn):
        @pl.when(lvl == 2)
        def _():
            fn(True)

        if i == 0:
            @pl.when(lvl == 1)
            def _():
                fn(False)

    def ly(i, full):
        return remote(part_of(ltv, i, full), part_of(ltg.at[qc, r], i, full), lys.at[i], ltr.at[qc, r, i], dev(t, c))

    def ly_do(i, op):
        @pl.when(d != 0)
        def _():
            by_level(i, level(t, r, qc, i), lambda full: op(ly(i, full)))

    def l_own(i):
        return pltpu.make_async_copy(part_of(ltv, i, True), part_of(ltg.at[qc, r], i, True), ltr.at[qc, r, i])

    def l_zero(q, rr, j):
        src = lt_in.at[pl.ds(0, ndiag), pl.ds(0, BLK)]
        return pltpu.make_async_copy(src, ltg.at[q, rr, pl.ds(0, ndiag), :, pl.ds(j * BLK, BLK)], s_ltz.at[q, rr, j])

    def l_zeros(op):
        @pl.loop(0, nr)
        def _(rr):
            for q in range(2):
                lvl = level(r, rr, q, 0)
                mine = jnp.logical_and(is_root, jnp.logical_and(rr == r, qc == q))
                for j in range(2):
                    @pl.when(jnp.logical_and(lvl < 2 - j, jnp.logical_not(mine)))
                    def _():
                        op(l_zero(q, rr, j))

    for n in range(L_BUF - 1):
        lin(n).start()
    for b in range(1, NSUM):
        lth[pl.ds(b * BLK, BLK), pl.ds(0, b * ch)] = jnp.zeros((BLK, b * ch), BF)

    @pl.loop(0, ntot)
    def _(n):
        lin(n).wait()

        @pl.when(n + L_BUF - 1 < ntot)
        def _():
            lin(n + L_BUF - 1).start()

        blk = lt_in[lax.rem(n, L_BUF)].T

        @pl.when(n < nt)
        def _():
            ltv[n] = blk

        @pl.when(n >= nt)
        def _():
            b, q = block_of(n, order)
            lth[pl.ds(pl.multiple_of(b * BLK, BLK), BLK), pl.ds(pl.multiple_of(q * ch, ch), ch)] = blk

        for i in range(L_CUT):
            @pl.when(n == cuts[i + 1] - 1)
            def _():
                @pl.when(is_root)
                def _():
                    l_own(i).start()

                ly_do(i, lambda cp: cp.start())

    lt_in[...] = jnp.zeros_like(lt_in)
    l_zeros(lambda cp: cp.start())
    for i in range(len(zeros)):
        zero_copy(i).start()

    @pl.when(is_root)
    def _():
        for b in range(nb):
            own_b(b).wait()
        for b in range(nb):
            own_b_out(b).start()

    on_ring = par == lax.rem(r, 2)

    def l_do(q, e, w, to, op):
        rr = mod(r + lax.rem(e, nr), nr)

        def go(i, full):
            ref = part_of(ltg.at[q, rr], i, full)
            op(remote(ref, ref, lts.at[e, q, w], ltr.at[q, rr, i], dev(r, to)))

        for i in range(L_CUT):
            @pl.when(e // nr == i)
            def _():
                by_level(i, level(r, rr, q, i), functools.partial(go, i))

    def l_send(q, e, w, to):
        l_do(q, e, w, to, lambda cp: cp.start())

    def l_wait(q, e):
        rr = mod(r + lax.rem(e, nr), nr)
        mine = jnp.logical_and(is_root, jnp.logical_and(rr == r, qc == q))

        def go(i, full):
            arrived(part_of(ltg.at[q, rr], i, full), ltr.at[q, rr, i])

        for i in range(L_CUT):
            @pl.when(e // nr == i)
            def _():
                by_level(i, jnp.where(mine, 2, level(r, rr, q, i)), functools.partial(go, i))

    right = mod(c + 2, nc)
    left = mod(c - 2, nc)
    def l_fwd(q, e, op):
        side = lax.rem(e, nr) // 2
        from_left = c == mod(r + nr * q + 2, nc)

        @pl.when(from_left == (side == 0))
        def _():
            l_do(q, e, 0, jnp.where(from_left, right, left), op)

    def l_stage0(e):
        l_wait(qc, e)
        l_send(qc, e, 0, right)
        l_send(qc, e, 1, left)
        l_send(qc, e, 2, sib)

    def l_stage1(e):
        for q in range(2):
            l_wait(q, e)
            l_fwd(q, e, lambda cp: cp.start())
            l_send(q, e, 2, sib)

    def l_stage2(e):
        l_wait(1 - qc, e)
        l_send(1 - qc, e, 2, sib)

    def l_stage3(e):
        for q in range(2):
            l_wait(q, e)

    bh = BLK // B_CUT

    def b_ref_of(v, lo, hi):
        return bc.at[v // B_CUT, pl.ds(lo, hi - lo), pl.ds(lax.rem(v, B_CUT) * bh, bh)]

    def b_send(v, lo, hi, ss, rs, dd):
        ref = b_ref_of(v, lo, hi)
        return remote(ref, ref, bys.at[v, ss], byr.at[v, rs], dev(row_of(dd), c))

    def b_wait(v, lo, hi, rs):
        arrived(b_ref_of(v, lo, hi), byr.at[v, rs])

    ja, jc = JA, JC
    b_moves = [(0, lambda v: b_send(v, 0, nc, 0, 0, 3)), (0, lambda v: b_send(v, ja, nc, 1, 0, 1)),
               (3, lambda v: b_send(v, 0, jc, 0, 0, 2)), (1, lambda v: b_send(v, jc, nc, 0, 1, 2)),
               (2, lambda v: b_send(v, 0, ja, 0, 1, 1))]

    mrow = SUM_UP
    prows = NSUM * BLK
    part_rows = ((mrow, prows - mrow), (0, mrow))

    def sum_send(o, part):
        lo, n = part_rows[part]
        to = row_of(mod(d - 1, nr)) if part == 0 else row_of(mod(d + 1, nr))
        dst = (prm if part == 0 else prp).at[o]
        return remote(pv.at[o, pl.ds(lo, n)], dst, prs.at[o, part], prr.at[o, part], dev(to, c))

    def sum_step(o, part, depth):
        lo, n = part_rows[part]
        land = (prm if part == 0 else prp).at[o]
        buf = rbm if part == 0 else rbp

        arrived(land, prr.at[o, part])
        cp = pltpu.make_async_copy(land, buf, s_rb.at[part])
        cp.start()
        cp.wait()

        @pl.loop(0, n // 64)
        def _(i):
            pv[o, pl.ds(lo + i * 64, 64)] = pv[o, pl.ds(lo + i * 64, 64)] + buf[pl.ds(i * 64, 64)]

        @pl.when(jnp.logical_not(is_root))
        def _():
            sum_send(o, part).start()

    def out_send(o, b, to):
        dst = db_ref.at[pl.ds((2 * b + qc) * BLK, BLK)]
        return remote(sv.at[o, pl.ds(b * BLK, BLK)], dst, dbs.at[o, b], dbr.at[2 * b + qc], dev(r, to))

    def out_local(o, b):
        dst = db_ref.at[pl.ds((2 * b + qc) * BLK, BLK)]
        return pltpu.make_async_copy(sv.at[o, pl.ds(b * BLK, BLK)], dst, dbr.at[2 * b + qc])

    def finish(o):
        @pl.loop(0, prows // 64)
        def _(i):
            sv[o, pl.ds(i * 64, 64)] = pv[o, pl.ds(i * 64, 64)].astype(BF)

        for b in range(NSUM):
            @pl.when(o == 0)
            def _():
                out_local(o, b).start()

            @pl.when(o != 0)
            def _():
                out_send(o, b, piece(o)).start()

    def partial(o):
        pv[o] = jnp.dot(lth[...], dxv[lax.rem(o, 2)], preferred_element_type=F32)

    offd = [next((n for n, x in enumerate(tail) if n >= ndiag and x[0] == b), nt) for b in range(NSUM, nb)]
    n2 = (nb - NSUM) * nr

    def t2_load(w, q, i):
        g, k = w // nr, lax.rem(w, 2)
        n = jnp.where(i == 0, g, table(g, offd) + i - 1)
        dst = ltb.at[k, pl.ds(q * BLK, BLK), pl.ds(pl.multiple_of(i * ch, ch), ch)]
        return pltpu.make_async_copy(ltg.at[q, lax.rem(w, nr), n], dst, s_ltb.at[k, q, i])

    def t2_loads(w, op):
        @pl.loop(0, nq - NSUM - w // nr)
        def _(i):
            for q in range(2):
                op(t2_load(w, q, i))

    def t2_start(w):
        t2_loads(w, lambda cp: cp.start())

    def t2_out(g):
        k = lax.rem(g, 2)
        return pltpu.make_async_copy(o2.at[k], db_ref.at[pl.ds((NSUM + g) * ch, ch)], s_o2.at[k])

    def t2_item(w):
        g, rr, k = w // nr, lax.rem(w, nr), lax.rem(w, 2)
        t2_loads(w, lambda cp: cp.wait())

        @pl.when(w + 1 < n2)
        def _():
            t2_start(w + 1)

        for gg in range(nb - NSUM):
            @pl.when(g == gg)
            def _():
                deep = (nq - NSUM - gg) * ch
                v = jnp.dot(ltb[k, :, pl.ds(0, deep)], dxtv[rr, pl.ds(gg * ch, deep)], preferred_element_type=F32)

                @pl.when(rr == 0)
                def _():
                    acc2[...] = v

                @pl.when(rr != 0)
                def _():
                    acc2[...] = acc2[...] + v

        @pl.when(rr == nr - 1)
        def _():
            @pl.when(g >= 2)
            def _():
                t2_out(g - 2).wait()
            o2[lax.rem(g, 2)] = acc2[...].astype(BF)
            t2_out(g).start()

    t3_order = [(b, q) for b in range(nb) for q in range(b, nq)]
    n3 = len(t3_order)
    t3_last = [max(n for n, (bb, _) in enumerate(t3_order) if bb == b) for b in range(nb)]

    def t3_load(n, o):
        b, q = block_of(n, t3_order)
        k = lax.rem(n, 2)
        rws = pl.ds(pl.multiple_of(q * ch, ch), ch)
        src = x_ref.at[rws] if o == 0 else dxg.at[mod(c + o, nc), rws]
        return pltpu.make_async_copy(src, dt.at[k, :, pl.ds(pl.multiple_of(mod(c + o, nc) * width, width), width)], s_dt.at[k, o])

    def bv_load(b, j):
        k = lax.rem(b, 2)
        return pltpu.make_async_copy(bc.at[b, j], bv.at[k, :, pl.ds(j * width, width)], s_bv.at[k, j])

    def t3_out(n):
        b, q = block_of(n, t3_order)
        k = lax.rem(n, 2)
        dst = dl_ref.at[pl.ds(pl.multiple_of(q * ch, ch), ch), pl.ds(pl.multiple_of(b * BLK, BLK), BLK)]
        return pltpu.make_async_copy(o3.at[k], dst, s_o3.at[k])

    def t3_item(n):
        b, q = block_of(n, t3_order)
        k = lax.rem(n, 2)
        for o in range(nc):
            t3_load(n, o).wait()

        @pl.when(n + 1 < n3)
        def _():
            for o in range(nc):
                t3_load(n + 1, o).start()

        @pl.when(q == b)
        def _():
            for j in range(nc):
                bv_load(b, j).wait()

        acc3[...] = lax.dot_general(dt[k], bv[lax.rem(b, 2)], (((1,), (1,)), ((), ())), preferred_element_type=F32)

        @pl.when(n >= 2)
        def _():
            t3_out(n - 2).wait()

        for i in range(ch // 128):
            pos = lax.broadcasted_iota(jnp.int32, (128, BLK), 0) + i * 128
            kpos = lax.broadcasted_iota(jnp.int32, (128, BLK), 1)
            rg = ((2 * q + i * 128 // BLK) * nr + r) * BLK + pos % BLK
            cg = (b * nc + c) * BLK + kpos
            o3[k, pl.ds(i * 128, 128)] = jnp.where(rg >= cg, acc3[pl.ds(i * 128, 128)], 0.0).astype(BF)
        t3_out(n).start()
    b_ready = [max(x[B_CUT * b + B_CUT - 1] for x in b_slot) for b in range(nb)]
    l_ready = [max(x[nr * i + nr - 1] for x in l_slot) for i in range(L_CUT)]
    t2_need = [l_ready[min(w // nr + 1, L_CUT - 1)] for w in range(n2)]

    def b_loads(slots):
        return [max(b_ready[b], T3_A - 1 if b < 2 else slots[t3_last[b - 2]]) for b in range(nb)]

    def earliest(begin, end, n, fits):
        found = []
        for first in range(begin, end):
            num = next((m for m in range(2, BLK) if fits(_line((first, m, 4), n))), None)
            if num is not None:
                found.append((_line((first, num, 4), n)[-1], first, num))
        _, first, num = min(found)
        return first, num, _line((first, num, 4), n)

    t2_first_slot, t2_num, t2_slots = earliest(T2_A, T2_A + 2, n2, lambda x: all(x[w] >= t2_need[min(w + 1, n2 - 1)] for w in range(n2)))
    t3_first_slot, t3_num, t3_slots = earliest(
        max(T3_A, b_ready[0] + 1), max(T3_A, b_ready[1]) + 2, n3,
        lambda x: all(a > y for a, y in zip((x[t3_last[b] + b - nb + 1] for b in range(nb)), b_loads(x))))
    bv_slots = b_loads(t3_slots)
    assert T2_A > max(l_ready[1], Y_EVENTS[6]) and Y_EVENTS[6] > max(Y_EVENTS[3:6])
    assert T3_A > max(load_x_at[-1], DX_EVENTS[-1])
    lists = ((SUM_X,) + sum_at, b_slot, l_slot)
    assert all(a < b for f in lists for x in f for a, b in zip(x[:-1], x[1:]))
    assert all(a < b for f in lists for y, z in zip(f[:-1], f[1:]) for a, b in zip(y, z))
    assert all(SUM_X[o - 2] < load_x_at[o] for o in range(2, nc))
    assert all(max(DX_EVENTS[o:o + 2]) <= load_x_at[o + 2] for o in (0, 2, 4))
    assert all(b_slot[0][B_CUT * b] <= sum_at[-1][b] for b in range(nb))
    slots = 1 + max(t3_slots[-1], t2_slots[-1], sum_at[-1][-1], b_ready[-1], l_ready[-1])

    down_depth = nr - 1 - d
    up_depth = mod(d - 1, nr)
    off_ring = jnp.logical_not(on_ring)

    events = []

    def event(slot, fn):
        events.append((slot, fn))

    def dx_event(i):
        p, h, ms = ev[i]
        dx_wait(p, h)
        for m in ms:
            m().start()

    def dx_rest():
        for m in own_list[4:]:
            m().start()

    def bx_event(b):
        bx_start(b)

    def y_first():
        dy_list[2]().start()
        dy_list[3]().start()

    def y_event(i):
        if i == 1:
            dy_wait(down, 0)
            dy_list[4]().start()
        elif i == 2:
            dy_wait(up, 1)
            dy_list[5]().start()
        elif i == 3:
            dy_wait(down, 1)
        elif i == 4:
            dy_wait(up, 0)
        else:
            dy_wait(opp, 0)
            dy_wait(opp, 1)

    def y_load(op):
        for i in range(nr):
            rr = mod(r + i, nr)
            src = x_ref.at[pl.ds(yrow0, 2 * yhalf)] if i == 0 else dxt.at[rr]
            op(pltpu.make_async_copy(src, dxtv.at[rr], s_dxt.at[i]))

    def t2_first():
        l_zeros(lambda cp: cp.wait())
        t2_start(0)
        y_load(lambda cp: cp.wait())

    def t3_first():
        for o in range(nc):
            t3_load(0, o).start()

    def bv_event(b):
        for j in range(nc):
            bv_load(b, j).start()

    for i in range(len(ev)):
        event(DX_EVENTS[i], functools.partial(dx_event, i))
    event(DX_SEND, dx_rest)
    for b in range(1, nb):
        event(bx_at[b], functools.partial(bx_event, b))
    event(Y_EVENTS[0], y_first)
    for i in range(1, 6):
        event(Y_EVENTS[i], functools.partial(y_event, i))
    event(Y_EVENTS[6], lambda: y_load(lambda cp: cp.start()))
    n_first = len(events)
    event(T2_A - 1, t2_first)
    event(T3_A - 1, t3_first)
    for b in range(nb):
        event(bv_slots[b], functools.partial(bv_event, b))
    masks = {}
    for i, (x, _) in enumerate(events):
        masks[x] = masks.get(x, 0) + (1 << i)

    def mask_of(s):
        m = jnp.int32(0)
        for x in sorted(masks):
            m = jnp.where(s == x, masks[x], m)
        return m

    def run_events(mask, lo, hi):
        part = sum(1 << i for i in range(lo, hi))

        @pl.when(jnp.bitwise_and(mask, part) != 0)
        def _():
            for i in range(lo, hi):
                @pl.when(jnp.bitwise_and(mask, 1 << i) != 0)
                def _():
                    events[i][1]()

    def b_due(v):
        @pl.when(is_root)
        def _():
            @pl.when(lax.rem(v, B_CUT) == 0)
            def _():
                @pl.loop(0, nc)
                def _(j):
                    arrived(bc.at[v // B_CUT, j], bxr.at[v // B_CUT, j])
            b_moves[0][1](v).start()
            b_moves[1][1](v).start()

        @pl.when(d == 3)
        def _():
            b_wait(v, 0, nc, 0)
            b_moves[2][1](v).start()

        @pl.when(d == 1)
        def _():
            b_wait(v, ja, nc, 0)
            b_moves[3][1](v).start()

        @pl.when(d == 2)
        def _():
            b_wait(v, 0, jc, 0)
            b_moves[4][1](v).start()
            b_wait(v, jc, nc, 1)

    def b_last(v):
        b_wait(v, 0, ja, 1)

    def l_due(e):
        @pl.when(is_root)
        def _():
            l_stage0(e)

        @pl.when(off_ring)
        def _():
            l_stage3(e)

        @pl.when(jnp.logical_and(on_ring, jnp.logical_not(is_root)))
        def _():
            l_stage1(e)

    def sum_due(o, part, depth):
        sum_step(o, part, depth)

    def load_due(o):
        p = piece(o)
        k = lax.rem(o, 2)

        @pl.when(k == 1)
        def _():
            dx_wait(p, 0)
            dx_wait(p, 1)

        @pl.when(o > 0)
        def _():
            pltpu.make_async_copy(dxg.at[p], dxv.at[k], s_dxv.at[k]).start()

    def part_due(o):
        load_x(0, lax.rem(o, 2)).wait()
        partial(o)
        for part, depth in ((0, down_depth), (1, up_depth)):
            @pl.when(depth == 0)
            def _():
                sum_send(o, part).start()

    def stage(lines, k):
        first = jnp.int32(slots)
        num = jnp.int32(0)
        for i, (f, m, _) in enumerate(lines):
            first = jnp.where(k == i, f, first)
            num = jnp.where(k == i, m, num)
        return lambda n: first + n * num // 4

    def listed(vals):
        return lambda n: table(n, vals + (slots,))

    def up_due(o):
        sum_due(o, 1, up_depth)

        @pl.when(is_root)
        def _():
            finish(o)

    none = jnp.int32(-1)
    flows = [(stage(L_LINES, jnp.where(is_root, 0, jnp.where(off_ring, 3, 1))), ne, l_due),
             (stage(L_LINES, jnp.where(is_root, 2, none)), ne, l_stage2),
             (stage(B_LINES, jnp.where(d == 0, 0, jnp.where(d == 2, 2, 1))), nv, b_due),
             (stage(B_LINES, jnp.where(d == 1, 3, none)), nv, b_last),
             (stage(SUM_LINES, down_depth - 1), nc, lambda o: sum_due(o, 0, down_depth)),
             (stage(SUM_LINES, up_depth - 1), nc, up_due),
             (listed(load_x_at), nc, load_due),
             (listed(SUM_X), nc, part_due)]
    work = [(lambda n: t2_first_slot + n * t2_num // 4, n2, t2_item), (lambda n: t3_first_slot + n * t3_num // 4, n3, t3_item)]

    def slot(s, carry):
        nxt = list(carry)
        mask = mask_of(s)
        run_events(mask, 0, n_first)

        def due(i, when, total, fn):
            n = nxt[i]
            hit = jnp.logical_and(n < total, when(n) == s)

            @pl.when(hit)
            def _():
                fn(n)

            nxt[i] = jnp.where(hit, n + 1, n)

        for i, (when, total, fn) in enumerate(flows):
            due(i, when, total, fn)
        run_events(mask, n_first, n_first + 2)
        for i, (when, total, fn) in enumerate(work):
            k = len(flows) + i

            def again(_, n):
                hit = jnp.logical_and(n < total, when(n) == s)

                @pl.when(hit)
                def _():
                    fn(n)

                return jnp.where(hit, n + 1, n)

            nxt[k] = lax.fori_loop(0, PER_SLOT, again, nxt[k])
        run_events(mask, n_first + 2, len(events))
        return tuple(nxt)

    lax.fori_loop(0, slots, slot, tuple(jnp.int32(0) for _ in range(len(flows) + len(work))))

    for g in (n2 // nr - 2, n2 // nr - 1):
        t2_out(g).wait()
    for n in (n3 - 2, n3 - 1):
        t3_out(n).wait()
    for i in range(len(zeros)):
        zero_copy(i).wait()
    for i in range(2 * NSUM):
        arrived(db_ref.at[pl.ds(i * BLK, BLK)], dbr.at[i])

    for cond, make, _ in sends:
        if cond is None:
            make().wait_send()
        else:
            @pl.when(cond)
            def _():
                make().wait_send()

    @pl.loop(0, nv)
    def _(v):
        for dd, make in b_moves:
            @pl.when(d == dd)
            def _():
                make(v).wait_send()

    def sent(cp):
        cp.wait_send()

    for i in range(L_CUT):
        ly_do(i, sent)

    @pl.loop(0, ne)
    def _(e):
        @pl.when(is_root)
        def _():
            l_do(qc, e, 0, right, sent)
            l_do(qc, e, 1, left, sent)
            l_do(qc, e, 2, sib, sent)
            l_do(1 - qc, e, 2, sib, sent)

        @pl.when(jnp.logical_and(on_ring, jnp.logical_not(is_root)))
        def _():
            for q in range(2):
                l_fwd(q, e, sent)
                l_do(q, e, 2, sib, sent)

    @pl.loop(0, 8)
    def _(o):
        @pl.when(jnp.logical_not(is_root))
        def _():
            for part in range(2):
                sum_send(o, part).wait_send()

        @pl.when(jnp.logical_and(is_root, o != 0))
        def _():
            for b in range(NSUM):
                out_send(o, b, piece(o)).wait_send()


def solution(mesh):
    nr = mesh.shape["row"]
    nc = mesh.shape["col"]
    spec = P(("batch", "row"), "col")

    def per_device(lower_tri, right_side, grad_out):
        rows, cols = lower_tri.shape
        width = right_side.shape[1]
        ch = 2 * BLK
        nq, nb = rows // ch, cols // BLK
        nt = sum(nq - b for b in range(NSUM, nb))
        ntot = sum(nq - b for b in range(nb))
        yrows = rows - NSUM * ch
        nzero = nb * (nb - 1) // 2
        sd = jax.ShapeDtypeStruct
        outs = (sd((rows, width), BF), sd((rows, cols), BF), sd((nc, rows, width), BF), sd((nb, nc, BLK, width), BF),
                sd((nr, yrows, width), BF), sd((2, nr, nt, BLK, ch), BF),
                sd((nc, NSUM * BLK - SUM_UP, width), F32), sd((nc, SUM_UP, width), F32))
        vm = pltpu.VMEM
        dma = pltpu.SemaphoreType.DMA
        scratch = [vm((L_BUF, ch, BLK), BF), vm((nt, BLK, ch), BF), vm((NSUM * BLK, rows), BF), vm((2, rows, width), BF), vm((nc, NSUM * BLK, width), F32),
                   vm((NSUM * BLK - SUM_UP, width), F32), vm((SUM_UP, width), F32), vm((nc, NSUM * BLK, width), BF),
                   vm((nr, yrows, width), BF), vm((2, ch, (nq - NSUM) * ch), BF), vm((ch, width), F32), vm((2, ch, width), BF),
                   vm((2, ch, nc * width), BF), vm((2, BLK, nc * width), BF), vm((ch, BLK), F32), vm((2, ch, BLK), BF),
                   dma((14,)), dma((nc, 2)), dma((nb, 2)), dma((nb, nc)), dma((nb * B_CUT, 2)), dma((nb * B_CUT, 2)),
                   dma((6,)), dma((nr, 2)), dma((L_CUT,)), dma((nr * L_CUT, 2, 3)), dma((2, nr, L_CUT)),
                   dma((nc, 2)), dma((nc, 2)), dma((nc, NSUM)), dma((2 * NSUM,)),
                   dma((2, nr, 2)), dma((L_BUF,)), dma((2,)), dma((2,)), dma((nr,)), dma((2, 2, nq - NSUM)), dma((2,)), dma((2, nc)), dma((2, nc)),
                   dma((2,)), dma((nzero,)), dma((nb,))]
        res = pl.pallas_call(
            functools.partial(_kernel, nr, nc),
            out_shape=outs,
            in_specs=[pl.BlockSpec(memory_space=pl.ANY)] * 3,
            out_specs=tuple(pl.BlockSpec(memory_space=pl.ANY) for _ in outs),
            scratch_shapes=scratch,
            compiler_params=pltpu.CompilerParams(collective_id=0, has_side_effects=True, vmem_limit_bytes=67043328),
            name="tri_backward",
        )(lower_tri, right_side, grad_out)
        return res[0], res[1]

    return jax.shard_map(per_device, mesh=mesh, in_specs=(spec, spec, spec), out_specs=(spec, spec), check_vma=False)
```

```python
import functools
import itertools

import jax
import jax.numpy as jnp
from jax import lax
from jax.experimental import pallas as pl
from jax.experimental.pallas import tpu as pltpu
from jax.sharding import PartitionSpec as P

BLK = 256
NSUM = 3
VMEM_BYTES = 67043328
BF = jnp.bfloat16
F32 = jnp.float32

LATE = 4
B_CUT = 4
L_CUT = 3
L_BUF = 4
DX_SEND = 14
DX_EVENTS = (17, 33, 30, 46, 59, 73)
SUM_X = (10, 11, 34, 36, 50, 53, 78, 86)
SUM_LINES = ((28, 41, 4), (44, 42, 4), (62, 35, 4), (74, 39, 4))
BX_LINE = (6, 31, 4)
B_LINES = ((25, 13, 4), (37, 15, 4), (73, 11, 4), (82, 10, 4))
L_LINES = ((45, 4, 4), (89, 11, 4), (90, 14, 4), (99, 11, 4))
Y_EVENTS = (12, 12, 21, 50, 51, 63, 64)
T2_A = 119
T3_A = 88
JA, JC, SUM_UP = 3,5,128


def _line(line, n):
    first, num, den = line
    return tuple(first + i * num // den for i in range(n))


def _round_lower(acc, out, b, q, row, col):
    part = BLK // 2
    for i in range(acc.shape[0] // part):
        pos = lax.broadcasted_iota(jnp.int32, (part, BLK), 0) + i * part
        rg = ((2 * q + i * part // BLK) * row[1] + row[0]) * BLK + pos % BLK
        cg = (b * col[1] + col[0]) * BLK + lax.broadcasted_iota(jnp.int32, (part, BLK), 1)
        out[pl.ds(i * part, part)] = jnp.where(rg >= cg, acc[pl.ds(i * part, part)], 0.0).astype(BF)


def _last_kernel(nr, nc, x_ref, dxg, bc, tiles_in, db_in, db_ref, dl_ref, xt, bt, tiles, dbv, acc, made, zero,
                 s_x, s_b, s_in, s_out, s_made, s_zero, s_db):
    rows, cols = dl_ref.shape
    width = x_ref.shape[1]
    ch = 2 * BLK
    nq, nb = rows // ch, cols // BLK
    r = lax.axis_index("row")
    c = lax.axis_index("col")
    early = [(b, q) for b in range(LATE) for q in range(b, nq)]
    late = [(b, q) for q in range(LATE, nq) for b in range(LATE, min(q + 1, nb))]
    above = [(b, q) for b in range(nb) for q in range(b)]

    def place(b, q):
        return dl_ref.at[pl.ds(pl.multiple_of(q * ch, ch), ch), pl.ds(pl.multiple_of(b * BLK, BLK), BLK)]

    def x_load(q, o):
        j = lax.rem(c + o, nc)
        rws = pl.ds(pl.multiple_of((LATE + q) * ch, ch), ch)
        src = x_ref.at[rws] if o == 0 else dxg.at[j, rws]
        return pltpu.make_async_copy(src, xt.at[q, :, pl.ds(pl.multiple_of(j * width, width), width)], s_x.at[q, o])

    def b_load(b, j):
        return pltpu.make_async_copy(bc.at[LATE + b, j], bt.at[b, :, pl.ds(j * width, width)], s_b.at[b, j])

    def tile_load(n):
        return pltpu.make_async_copy(tiles_in.at[n], tiles.at[n], s_in.at[n])

    def tile_store(n):
        return pltpu.make_async_copy(tiles.at[n], place(*early[n]), s_out.at[n])

    def zero_store(n):
        return pltpu.make_async_copy(zero, place(*above[n]), s_zero.at[n])

    db_load = pltpu.make_async_copy(db_in, dbv, s_db.at[0])
    db_store = pltpu.make_async_copy(dbv, db_ref, s_db.at[1])
    for i in range(nq - LATE):
        for o in range(nc):
            x_load(i, o).start()
        for j in range(nc):
            b_load(i, j).start()
    for n in range(len(early)):
        tile_load(n).start()
    db_load.start()
    zero[...] = jnp.zeros_like(zero)
    for n in range(len(above)):
        zero_store(n).start()

    def of(n, vals):
        v = jnp.int32(vals[0])
        for i in range(1, len(vals)):
            v = jnp.where(n >= i, vals[i], v)
        return v

    def made_store(n):
        return pltpu.make_async_copy(made.at[n], place(of(n, [b for b, _ in late]), of(n, [q for _, q in late])), s_made.at[n])

    @pl.loop(0, len(late))
    def _(n):
        b = of(n, [b for b, _ in late])
        q = of(n, [q for _, q in late])

        @pl.when(b == LATE)
        def _():
            for o in range(nc):
                x_load(q - LATE, o).wait()

        @pl.when(b == q)
        def _():
            for j in range(nc):
                b_load(b - LATE, j).wait()

        acc[...] = lax.dot_general(xt[q - LATE], bt[b - LATE], (((1,), (1,)), ((), ())), preferred_element_type=F32)
        _round_lower(acc, made.at[n], b, q, (r, nr), (c, nc))
        made_store(n).start()

        @pl.when(n == len(late) // 2)
        def _():
            for i in range(len(early)):
                tile_load(i).wait()
                tile_store(i).start()
            db_load.wait()
            db_store.start()

    for n in range(len(late)):
        made_store(n).wait()
    for n in range(len(early)):
        tile_store(n).wait()
    for n in range(len(above)):
        zero_store(n).wait()
    db_store.wait()


def _kernel(nr, nc, l_ref, b_ref, x_ref, db_ref, dl_ref, dxg, bc, dxt, ltg, prm, prp,
            lt_in, ltv, lth, dxv, pv, rbm, rbp, sv, dxtv, ltb, acc2, o2, dt, bv, acc3, o3,
            dxs, dxr, bxs, bxr, bys, byr, dys, dyr, lys, lts, ltr, prs, prr, dbs, dbr,
            s_ltz, s_lin, s_dxv, s_rb, s_dxt, s_ltb, s_o2, s_dt, s_bv, s_o3, s_own):
    rows, cols = l_ref.shape
    width = x_ref.shape[1]
    ch = 2 * BLK
    nq = rows // ch
    nb = cols // BLK
    tail = [(b, b) for b in range(NSUM, nb)] + [(b, q) for b in range(NSUM, nb) for q in range(b + 1, nq)]
    ndiag = nb - NSUM
    head = [(b, q) for b in range(NSUM) for q in range(b, nq)]
    nt = len(tail)
    off = {}
    for n, (b, q) in enumerate(tail + head):
        off.setdefault(b, n)
    half = rows // 2
    yrow0 = NSUM * ch
    yhalf = (rows - yrow0) // 2
    cuts = [n for n in range(nt) if n in (0, ndiag) or tail[n - 1][0] != tail[n][0] and n > ndiag][:L_CUT] + [nt]

    nv = nb * B_CUT
    ne = nr * L_CUT
    load_x_at = tuple(max(x - 1, 0) for x in SUM_X)
    sum_at = tuple(_line(x, nc) for x in SUM_LINES)
    bx_at = _line(BX_LINE, nb)
    b_slot = tuple(_line(x, nv) for x in B_LINES)
    l_slot = tuple(_line(x, ne) for x in L_LINES)

    z = lax.axis_index("batch")
    r = lax.axis_index("row")
    c = lax.axis_index("col")

    def dev(row, col):
        return (z, row, col)

    def remote(src, dst, ss, rs, to):
        return pltpu.make_async_remote_copy(src, dst, ss, rs, device_id=to, device_id_type=pl.DeviceIdType.MESH)

    def arrived(dst, sem):
        pltpu.make_async_copy(dst, dst, sem).wait()

    def mod(v, m):
        return lax.rem(v + 4 * m, m)

    par = lax.rem(c, 2)
    eps = 1 - 2 * par
    sib = c + eps
    far = mod(c + 4, nc)
    first = mod(c - 2 * eps, nc)
    second = mod(c + 2 * eps, nc)
    hf = par
    hs = 1 - par
    t = lax.rem(c, nr)
    sg = 1 - 2 * lax.rem(t, 2)
    d = mod((r - t) * sg, nr)
    is_root = d == 0
    qc = c // nr

    def row_of(dd):
        return mod(t + sg * dd, nr)

    def piece(o):
        vals = (0, 1, -2, 3, 2, -1, 4, 5)
        v = jnp.int32(vals[0])
        for i in range(1, 8):
            v = jnp.where(o == i, vals[i], v)
        return mod(c + eps * v, nc)

    def table(n, vals):
        v = jnp.int32(vals[0])
        for i in range(1, len(vals)):
            if vals[i] != vals[i - 1]:
                v = jnp.where(n >= i, vals[i], v)
        return v

    def summed(u):
        if isinstance(u, int):
            return u % (nc - 1) + 1 if u else 0
        return jnp.where(u == 0, 0, lax.rem(u, nc - 1) + 1)

    def block_of(n, order):
        return table(n, [b for b, _ in order]), table(n, [q for _, q in order])

    bar = pltpu.get_barrier_semaphore()
    for k in range(1, nc):
        pl.semaphore_signal(bar, inc=1, device_id=dev(r, mod(c + k, nc)), device_id_type=pl.DeviceIdType.MESH)
    for k in range(1, nr):
        pl.semaphore_signal(bar, inc=1, device_id=dev(mod(r + k, nr), c), device_id_type=pl.DeviceIdType.MESH)
    pl.semaphore_wait(bar, nc + nr - 2)

    sends = []

    def note(cond, make, grid=None):
        sends.append((cond, make, grid))

    def bx(b, q):
        src = b_ref.at[pl.ds((2 * b + q) * BLK, BLK)]
        return remote(src, bc.at[b, c], bxs.at[b, q], bxr.at[b, c], dev(r, r + nr * q))

    def bx_start(b):
        for q in range(2):
            @pl.when(c != r + nr * q)
            def _():
                bx(b, q).start()

    for b in range(nb):
        for q in range(2):
            note(c != r + nr * q, functools.partial(bx, b, q))

    def dx_own(h, to, i):
        src = x_ref.at[pl.ds(h * half, half)]
        return remote(src, dxg.at[c, pl.ds(h * half, half)], dxs.at[i], dxr.at[c, h], dev(r, to))

    def dx_fwd(p, h, to, i):
        ref = dxg.at[p, pl.ds(h * half, half)]
        return remote(ref, ref, dxs.at[i], dxr.at[p, h], dev(r, to))

    def dx_wait(p, h):
        arrived(dxg.at[p, pl.ds(h * half, half)], dxr.at[p, h])

    dx_id = itertools.count()
    own_list = [functools.partial(dx_own, hf, second, next(dx_id)), functools.partial(dx_own, hf, sib, next(dx_id)),
                functools.partial(dx_own, hs, second, next(dx_id)), functools.partial(dx_own, hs, sib, next(dx_id)),
                functools.partial(dx_own, hs, first, next(dx_id)), functools.partial(dx_own, hf, first, next(dx_id))]
    ev = [(first, hf, [functools.partial(dx_fwd, first, hf, second, next(dx_id)), functools.partial(dx_fwd, first, hf, sib, next(dx_id))]),
          (first, hs, [functools.partial(dx_fwd, first, hs, sib, next(dx_id))]),
          (second, hs, [functools.partial(dx_fwd, second, hs, first, next(dx_id)), functools.partial(dx_fwd, second, hs, sib, next(dx_id))]),
          (second, hf, [functools.partial(dx_fwd, second, hf, sib, next(dx_id))]),
          (far, hf, [functools.partial(dx_fwd, far, hf, sib, next(dx_id))]),
          (far, hs, [functools.partial(dx_fwd, far, hs, sib, next(dx_id))])]
    for m in own_list:
        note(None, m)
    for _, _, ms in ev:
        for m in ms:
            note(None, m)

    up = mod(r + 1, nr)
    down = mod(r + nr - 1, nr)
    opp = mod(r + 2, nr)

    def dy_own(h, to, i):
        src = x_ref.at[pl.ds(yrow0 + h * yhalf, yhalf)]
        return remote(src, dxt.at[r, pl.ds(h * yhalf, yhalf)], dys.at[i], dyr.at[r, h], dev(to, c))

    def dy_fwd(p, h, to, i):
        ref = dxt.at[p, pl.ds(h * yhalf, yhalf)]
        return remote(ref, ref, dys.at[i], dyr.at[p, h], dev(to, c))

    def dy_wait(p, h):
        arrived(dxt.at[p, pl.ds(h * yhalf, yhalf)], dyr.at[p, h])

    dy_id = itertools.count()
    dy_list = [functools.partial(dy_own, 0, up, next(dy_id)), functools.partial(dy_own, 1, down, next(dy_id)),
               functools.partial(dy_own, 1, up, next(dy_id)), functools.partial(dy_own, 0, down, next(dy_id)),
               functools.partial(dy_fwd, down, 0, up, next(dy_id)), functools.partial(dy_fwd, up, 1, down, next(dy_id))]
    for m in dy_list:
        note(None, m)

    own_list[0]().start()
    own_list[1]().start()
    bx_start(0)
    own_list[2]().start()
    own_list[3]().start()
    dy_list[0]().start()
    dy_list[1]().start()

    def load_x(o, slot):
        return pltpu.make_async_copy(x_ref, dxv.at[slot], s_dxv.at[slot])

    load_x(0, 0).start()

    def own_b(b):
        return pltpu.make_async_copy(b_ref.at[pl.ds((2 * b + qc) * BLK, BLK)], sv.at[summed(b), pl.ds(0, BLK)], s_own.at[b])

    def own_b_out(b):
        return pltpu.make_async_copy(sv.at[summed(b), pl.ds(0, BLK)], bc.at[b, c], bxr.at[b, c])

    @pl.when(is_root)
    def _():
        for b in range(nb):
            own_b(b).start()

    order = tail + head
    ntot = len(order)

    def lin(n):
        b, q = block_of(n, order)
        src = l_ref.at[pl.ds(pl.multiple_of(q * ch, ch), ch), pl.ds(pl.multiple_of(b * BLK, BLK), BLK)]
        return pltpu.make_async_copy(src, lt_in.at[lax.rem(n, L_BUF)], s_lin.at[lax.rem(n, L_BUF)])

    def part_of(ref, i, full):
        n = cuts[i + 1] - cuts[i]
        return ref.at[pl.ds(cuts[i], n)] if full else ref.at[pl.ds(cuts[i], n), :, pl.ds(BLK, BLK)]

    def level(home, src_row, q, i):
        return jnp.where(src_row >= home, 2, 1) - q if i == 0 else jnp.int32(2)

    def by_level(i, lvl, fn):
        @pl.when(lvl == 2)
        def _():
            fn(True)

        if i == 0:
            @pl.when(lvl == 1)
            def _():
                fn(False)

    def ly(i, full):
        return remote(part_of(ltv, i, full), part_of(ltg.at[qc, r], i, full), lys.at[i], ltr.at[qc, r, i], dev(t, c))

    def ly_do(i, op):
        @pl.when(d != 0)
        def _():
            by_level(i, level(t, r, qc, i), lambda full: op(ly(i, full)))

    def l_own(i):
        return pltpu.make_async_copy(part_of(ltv, i, True), part_of(ltg.at[qc, r], i, True), ltr.at[qc, r, i])

    def l_zero(q, rr, j):
        src = lt_in.at[pl.ds(0, ndiag), pl.ds(0, BLK)]
        return pltpu.make_async_copy(src, ltg.at[q, rr, pl.ds(0, ndiag), :, pl.ds(j * BLK, BLK)], s_ltz.at[q, rr, j])

    def l_zeros(op):
        @pl.loop(0, nr)
        def _(rr):
            for q in range(2):
                lvl = level(r, rr, q, 0)
                mine = jnp.logical_and(is_root, jnp.logical_and(rr == r, qc == q))
                for j in range(2):
                    @pl.when(jnp.logical_and(lvl < 2 - j, jnp.logical_not(mine)))
                    def _():
                        op(l_zero(q, rr, j))

    for n in range(L_BUF - 1):
        lin(n).start()
    for b in range(1, NSUM):
        lth[pl.ds(b * BLK, BLK), pl.ds(0, b * ch)] = jnp.zeros((BLK, b * ch), BF)

    @pl.loop(0, ntot)
    def _(n):
        lin(n).wait()

        @pl.when(n + L_BUF - 1 < ntot)
        def _():
            lin(n + L_BUF - 1).start()

        blk = lt_in[lax.rem(n, L_BUF)].T

        @pl.when(n < nt)
        def _():
            ltv[n] = blk

        @pl.when(n >= nt)
        def _():
            b, q = block_of(n, order)
            lth[pl.ds(pl.multiple_of(b * BLK, BLK), BLK), pl.ds(pl.multiple_of(q * ch, ch), ch)] = blk

        for i in range(L_CUT):
            @pl.when(n == cuts[i + 1] - 1)
            def _():
                @pl.when(is_root)
                def _():
                    l_own(i).start()

                ly_do(i, lambda cp: cp.start())

    lt_in[...] = jnp.zeros_like(lt_in)
    l_zeros(lambda cp: cp.start())

    @pl.when(is_root)
    def _():
        for b in range(nb):
            own_b(b).wait()
        for b in range(nb):
            own_b_out(b).start()

    on_ring = par == lax.rem(r, 2)

    def l_do(q, e, w, to, op):
        rr = mod(r + lax.rem(e, nr), nr)

        def go(i, full):
            ref = part_of(ltg.at[q, rr], i, full)
            op(remote(ref, ref, lts.at[e, q, w], ltr.at[q, rr, i], dev(r, to)))

        for i in range(L_CUT):
            @pl.when(e // nr == i)
            def _():
                by_level(i, level(r, rr, q, i), functools.partial(go, i))

    def l_send(q, e, w, to):
        l_do(q, e, w, to, lambda cp: cp.start())

    def l_wait(q, e):
        rr = mod(r + lax.rem(e, nr), nr)
        mine = jnp.logical_and(is_root, jnp.logical_and(rr == r, qc == q))

        def go(i, full):
            arrived(part_of(ltg.at[q, rr], i, full), ltr.at[q, rr, i])

        for i in range(L_CUT):
            @pl.when(e // nr == i)
            def _():
                by_level(i, jnp.where(mine, 2, level(r, rr, q, i)), functools.partial(go, i))

    right = mod(c + 2, nc)
    left = mod(c - 2, nc)
    def l_fwd(q, e, op):
        side = lax.rem(e, nr) // 2
        from_left = c == mod(r + nr * q + 2, nc)

        @pl.when(from_left == (side == 0))
        def _():
            l_do(q, e, 0, jnp.where(from_left, right, left), op)

    def l_stage0(e):
        l_wait(qc, e)
        l_send(qc, e, 0, right)
        l_send(qc, e, 1, left)
        l_send(qc, e, 2, sib)

    def l_stage1(e):
        for q in range(2):
            l_wait(q, e)
            l_fwd(q, e, lambda cp: cp.start())
            l_send(q, e, 2, sib)

    def l_stage2(e):
        l_wait(1 - qc, e)
        l_send(1 - qc, e, 2, sib)

    def l_stage3(e):
        for q in range(2):
            l_wait(q, e)

    bh = BLK // B_CUT

    def b_ref_of(v, lo, hi):
        return bc.at[v // B_CUT, pl.ds(lo, hi - lo), pl.ds(lax.rem(v, B_CUT) * bh, bh)]

    def b_send(v, lo, hi, ss, rs, dd):
        ref = b_ref_of(v, lo, hi)
        return remote(ref, ref, bys.at[v, ss], byr.at[v, rs], dev(row_of(dd), c))

    def b_wait(v, lo, hi, rs):
        arrived(b_ref_of(v, lo, hi), byr.at[v, rs])

    ja, jc = JA, JC
    b_moves = [(0, lambda v: b_send(v, 0, nc, 0, 0, 3)), (0, lambda v: b_send(v, ja, nc, 1, 0, 1)),
               (3, lambda v: b_send(v, 0, jc, 0, 0, 2)), (1, lambda v: b_send(v, jc, nc, 0, 1, 2)),
               (2, lambda v: b_send(v, 0, ja, 0, 1, 1))]

    mrow = SUM_UP
    prows = NSUM * BLK
    part_rows = ((mrow, prows - mrow), (0, mrow))

    def sum_send(o, part):
        lo, n = part_rows[part]
        to = row_of(mod(d - 1, nr)) if part == 0 else row_of(mod(d + 1, nr))
        dst = (prm if part == 0 else prp).at[o]
        return remote(pv.at[o, pl.ds(lo, n)], dst, prs.at[o, part], prr.at[o, part], dev(to, c))

    def sum_step(o, part, depth):
        lo, n = part_rows[part]
        land = (prm if part == 0 else prp).at[o]
        buf = rbm if part == 0 else rbp

        arrived(land, prr.at[o, part])
        cp = pltpu.make_async_copy(land, buf, s_rb.at[part])
        cp.start()
        cp.wait()

        @pl.loop(0, n // 64)
        def _(i):
            pv[o, pl.ds(lo + i * 64, 64)] = pv[o, pl.ds(lo + i * 64, 64)] + buf[pl.ds(i * 64, 64)]

        @pl.when(jnp.logical_not(is_root))
        def _():
            sum_send(o, part).start()

    def out_send(o, b, to):
        dst = db_ref.at[pl.ds((2 * b + qc) * BLK, BLK)]
        return remote(sv.at[o, pl.ds(b * BLK, BLK)], dst, dbs.at[o, b], dbr.at[2 * b + qc], dev(r, to))

    def out_local(o, b):
        dst = db_ref.at[pl.ds((2 * b + qc) * BLK, BLK)]
        return pltpu.make_async_copy(sv.at[o, pl.ds(b * BLK, BLK)], dst, dbr.at[2 * b + qc])

    def finish(o):
        @pl.loop(0, prows // 64)
        def _(i):
            sv[o, pl.ds(i * 64, 64)] = pv[o, pl.ds(i * 64, 64)].astype(BF)

        for b in range(NSUM):
            @pl.when(o == 0)
            def _():
                out_local(o, b).start()

            @pl.when(o != 0)
            def _():
                out_send(o, b, piece(o)).start()

    def partial(o):
        pv[o] = jnp.dot(lth[...], dxv[lax.rem(o, 2)], preferred_element_type=F32)

    offd = [next((n for n, x in enumerate(tail) if n >= ndiag and x[0] == b), nt) for b in range(NSUM, nb)]
    n2 = (nb - NSUM) * nr

    def t2_load(w, q, i):
        g, k = w // nr, lax.rem(w, 2)
        n = jnp.where(i == 0, g, table(g, offd) + i - 1)
        dst = ltb.at[k, pl.ds(q * BLK, BLK), pl.ds(pl.multiple_of(i * ch, ch), ch)]
        return pltpu.make_async_copy(ltg.at[q, lax.rem(w, nr), n], dst, s_ltb.at[k, q, i])

    def t2_loads(w, op):
        @pl.loop(0, nq - NSUM - w // nr)
        def _(i):
            for q in range(2):
                op(t2_load(w, q, i))

    def t2_start(w):
        t2_loads(w, lambda cp: cp.start())

    def t2_out(g):
        k = lax.rem(g, 2)
        return pltpu.make_async_copy(o2.at[k], db_ref.at[pl.ds((NSUM + g) * ch, ch)], s_o2.at[k])

    def t2_item(w):
        g, rr, k = w // nr, lax.rem(w, nr), lax.rem(w, 2)
        t2_loads(w, lambda cp: cp.wait())

        @pl.when(w + 1 < n2)
        def _():
            t2_start(w + 1)

        for gg in range(nb - NSUM):
            @pl.when(g == gg)
            def _():
                deep = (nq - NSUM - gg) * ch
                v = jnp.dot(ltb[k, :, pl.ds(0, deep)], dxtv[rr, pl.ds(gg * ch, deep)], preferred_element_type=F32)

                @pl.when(rr == 0)
                def _():
                    acc2[...] = v

                @pl.when(rr != 0)
                def _():
                    acc2[...] = acc2[...] + v

        @pl.when(rr == nr - 1)
        def _():
            @pl.when(g >= 2)
            def _():
                t2_out(g - 2).wait()
            o2[lax.rem(g, 2)] = acc2[...].astype(BF)
            t2_out(g).start()

    t3_order = [(b, q) for b in range(LATE) for q in range(b, nq)]
    n3 = len(t3_order)
    t3_last = [max(n for n, (bb, _) in enumerate(t3_order) if bb == b) for b in range(LATE)]

    def t3_load(n, o):
        b, q = block_of(n, t3_order)
        k = lax.rem(n, 2)
        rws = pl.ds(pl.multiple_of(q * ch, ch), ch)
        src = x_ref.at[rws] if o == 0 else dxg.at[mod(c + o, nc), rws]
        return pltpu.make_async_copy(src, dt.at[k, :, pl.ds(pl.multiple_of(mod(c + o, nc) * width, width), width)], s_dt.at[k, o])

    def bv_load(b, j):
        k = lax.rem(b, 2)
        return pltpu.make_async_copy(bc.at[b, j], bv.at[k, :, pl.ds(j * width, width)], s_bv.at[k, j])

    def t3_out(n):
        k = lax.rem(n, 2)
        return pltpu.make_async_copy(o3.at[k], dl_ref.at[n], s_o3.at[k])

    def t3_item(n):
        b, q = block_of(n, t3_order)
        k = lax.rem(n, 2)
        for o in range(nc):
            t3_load(n, o).wait()

        @pl.when(n + 1 < n3)
        def _():
            for o in range(nc):
                t3_load(n + 1, o).start()

        @pl.when(q == b)
        def _():
            for j in range(nc):
                bv_load(b, j).wait()

        acc3[...] = lax.dot_general(dt[k], bv[lax.rem(b, 2)], (((1,), (1,)), ((), ())), preferred_element_type=F32)

        @pl.when(n >= 2)
        def _():
            t3_out(n - 2).wait()

        _round_lower(acc3, o3.at[k], b, q, (r, nr), (c, nc))
        t3_out(n).start()
    b_ready = [max(x[B_CUT * b + B_CUT - 1] for x in b_slot) for b in range(nb)]
    l_ready = [max(x[nr * i + nr - 1] for x in l_slot) for i in range(L_CUT)]
    t2_need = [l_ready[min(w // nr + 1, L_CUT - 1)] for w in range(n2)]

    def packed(start, ready):
        out = []
        for n in range(len(ready)):
            out.append(max(start, ready[n], out[-1] + 1 if out else 0))
        return out

    t2_slots = packed(T2_A, t2_need[1:] + t2_need[-1:])
    t3_slots, bv_slots = [], []
    for b in range(LATE):
        bv_slots.append(max(b_ready[b], T3_A - 1 if b < 2 else t3_slots[t3_last[b - 2]]))
        t3_slots = packed(T3_A, t3_slots + [bv_slots[b] + 1] * (nq - b))
    assert T2_A > max(l_ready[1], Y_EVENTS[6]) and Y_EVENTS[6] > max(Y_EVENTS[3:6])
    assert T3_A > max(load_x_at[-1], DX_EVENTS[-1])
    lists = (sum_at, b_slot, l_slot)
    assert all(a < b for f in lists + ((SUM_X,),) for x in f for a, b in zip(x[:-1], x[1:]))
    assert all(sum_at[0][u] > SUM_X[summed(u)] for u in range(nc))
    assert all(a < b for f in lists for y, z in zip(f[:-1], f[1:]) for a, b in zip(y, z))
    assert all(SUM_X[o - 2] < load_x_at[o] for o in range(2, nc))
    assert all(max(DX_EVENTS[o:o + 2]) <= load_x_at[o + 2] for o in (0, 2, 4))
    assert all(b_slot[0][B_CUT * b] <= sum_at[-1][b] for b in range(nb))
    slots = 1 + max(t3_slots[-1], t2_slots[-1], sum_at[-1][-1], b_ready[-1], l_ready[-1])

    down_depth = nr - 1 - d
    up_depth = mod(d - 1, nr)
    off_ring = jnp.logical_not(on_ring)

    def listed(vals):
        return lambda n: table(n, tuple(vals) + (slots,))

    events = []

    def event(slot, fn):
        events.append((slot, fn))

    def dx_event(i):
        p, h, ms = ev[i]
        dx_wait(p, h)
        for m in ms:
            m().start()

    def dx_rest():
        for m in own_list[4:]:
            m().start()

    def bx_event(b):
        bx_start(b)

    def y_first():
        dy_list[2]().start()
        dy_list[3]().start()

    def y_event(i):
        if i == 1:
            dy_wait(down, 0)
            dy_list[4]().start()
        elif i == 2:
            dy_wait(up, 1)
            dy_list[5]().start()
        elif i == 3:
            dy_wait(down, 1)
        elif i == 4:
            dy_wait(up, 0)
        else:
            dy_wait(opp, 0)
            dy_wait(opp, 1)

    def y_load(op):
        for i in range(nr):
            rr = mod(r + i, nr)
            src = x_ref.at[pl.ds(yrow0, 2 * yhalf)] if i == 0 else dxt.at[rr]
            op(pltpu.make_async_copy(src, dxtv.at[rr], s_dxt.at[i]))

    def t2_first():
        l_zeros(lambda cp: cp.wait())
        t2_start(0)
        y_load(lambda cp: cp.wait())

    def t3_first():
        for o in range(nc):
            t3_load(0, o).start()

    def bv_event(b):
        for j in range(nc):
            bv_load(b, j).start()

    for i in range(len(ev)):
        event(DX_EVENTS[i], functools.partial(dx_event, i))
    event(DX_SEND, dx_rest)
    for b in range(1, nb):
        event(bx_at[b], functools.partial(bx_event, b))
    event(Y_EVENTS[0], y_first)
    for i in range(1, 6):
        event(Y_EVENTS[i], functools.partial(y_event, i))
    event(Y_EVENTS[6], lambda: y_load(lambda cp: cp.start()))
    n_first = len(events)
    event(T2_A - 1, t2_first)
    event(T3_A - 1, t3_first)
    for b in range(LATE):
        event(bv_slots[b], functools.partial(bv_event, b))

    def event_flow(lo, hi):
        part = sorted(range(lo, hi), key=lambda i: events[i][0])
        at = sorted({events[i][0] for i in part})
        masks = [sum(1 << (i - lo) for i in part if events[i][0] == x) for x in at]

        def run(k):
            mask = table(k, masks)
            for i in range(lo, hi):
                @pl.when(jnp.bitwise_and(mask, 1 << (i - lo)) != 0)
                def _():
                    events[i][1]()

        return listed(at), len(at), run

    def b_due(v):
        @pl.when(is_root)
        def _():
            @pl.when(lax.rem(v, B_CUT) == 0)
            def _():
                @pl.loop(0, nc)
                def _(j):
                    arrived(bc.at[v // B_CUT, j], bxr.at[v // B_CUT, j])
            b_moves[0][1](v).start()
            b_moves[1][1](v).start()

        @pl.when(d == 3)
        def _():
            b_wait(v, 0, nc, 0)
            b_moves[2][1](v).start()

        @pl.when(d == 1)
        def _():
            b_wait(v, ja, nc, 0)
            b_moves[3][1](v).start()

        @pl.when(d == 2)
        def _():
            b_wait(v, 0, jc, 0)
            b_moves[4][1](v).start()
            b_wait(v, jc, nc, 1)

    def b_last(v):
        b_wait(v, 0, ja, 1)

    def l_due(e):
        @pl.when(is_root)
        def _():
            l_stage0(e)

        @pl.when(off_ring)
        def _():
            l_stage3(e)

        @pl.when(jnp.logical_and(on_ring, jnp.logical_not(is_root)))
        def _():
            l_stage1(e)

    def sum_due(u, part, depth):
        o = summed(u)

        @pl.when(depth == 0)
        def _():
            sum_send(o, part).start()

        @pl.when(depth > 0)
        def _():
            sum_step(o, part, depth)

    def load_due(o):
        p = piece(o)
        k = lax.rem(o, 2)

        @pl.when(k == 1)
        def _():
            dx_wait(p, 0)
            dx_wait(p, 1)

        @pl.when(o > 0)
        def _():
            pltpu.make_async_copy(dxg.at[p], dxv.at[k], s_dxv.at[k]).start()

    def part_due(o):
        load_x(0, lax.rem(o, 2)).wait()
        partial(o)

    def stage(lines, k, total):
        first = jnp.int32(slots)
        num = jnp.int32(0)
        for i, (f, m, _) in enumerate(lines):
            first = jnp.where(k == i, f, first)
            num = jnp.where(k == i, m, num)
        return lambda n: jnp.where(n < total, first + n * num // 4, slots)

    def up_due(u):
        sum_due(u, 1, up_depth)

        @pl.when(is_root)
        def _():
            finish(summed(u))

    none = jnp.int32(-1)
    flows = [event_flow(0, n_first)[::2],
             (stage(L_LINES, jnp.where(is_root, 0, jnp.where(off_ring, 3, 1)), ne), l_due),
             (stage(L_LINES, jnp.where(is_root, 2, none), ne), l_stage2),
             (stage(B_LINES, jnp.where(d == 0, 0, jnp.where(d == 2, 2, 1)), nv), b_due),
             (stage(B_LINES, jnp.where(d == 1, 3, none), nv), b_last),
             (stage(SUM_LINES, down_depth, nc), lambda u: sum_due(u, 0, down_depth)),
             (stage(SUM_LINES, up_depth, nc), up_due),
             (listed(load_x_at), load_due),
             (listed(SUM_X), part_due),
             event_flow(n_first, n_first + 2)[::2],
             (listed(t2_slots), t2_item), (listed(t3_slots), t3_item), event_flow(n_first + 2, len(events))[::2]]

    def slot(s, carry):
        nxt = []
        for (when, fn), (n, at) in zip(flows, carry):
            def go(n, fn=fn, when=when):
                fn(n)
                return n + 1, when(n + 1)

            def stay(n, at=at):
                return n, at

            nxt.append(lax.cond(at == s, go, stay, n))
        return tuple(nxt)

    lax.fori_loop(0, slots, slot, tuple((jnp.int32(0), jnp.int32(when(jnp.int32(0)))) for when, _ in flows))

    for g in (n2 // nr - 2, n2 // nr - 1):
        t2_out(g).wait()
    for n in (n3 - 2, n3 - 1):
        t3_out(n).wait()
    for i in range(2 * NSUM):
        arrived(db_ref.at[pl.ds(i * BLK, BLK)], dbr.at[i])

    for cond, make, _ in sends:
        if cond is None:
            make().wait_send()
        else:
            @pl.when(cond)
            def _():
                make().wait_send()

    @pl.loop(0, nv)
    def _(v):
        for dd, make in b_moves:
            @pl.when(d == dd)
            def _():
                make(v).wait_send()

    def sent(cp):
        cp.wait_send()

    for i in range(L_CUT):
        ly_do(i, sent)

    @pl.loop(0, ne)
    def _(e):
        @pl.when(is_root)
        def _():
            l_do(qc, e, 0, right, sent)
            l_do(qc, e, 1, left, sent)
            l_do(qc, e, 2, sib, sent)
            l_do(1 - qc, e, 2, sib, sent)

        @pl.when(jnp.logical_and(on_ring, jnp.logical_not(is_root)))
        def _():
            for q in range(2):
                l_fwd(q, e, sent)
                l_do(q, e, 2, sib, sent)

    @pl.loop(0, 8)
    def _(o):
        @pl.when(jnp.logical_not(is_root))
        def _():
            for part in range(2):
                sum_send(o, part).wait_send()

        @pl.when(jnp.logical_and(is_root, o != 0))
        def _():
            for b in range(NSUM):
                out_send(o, b, piece(o)).wait_send()


def solution(mesh):
    nr = mesh.shape["row"]
    nc = mesh.shape["col"]
    spec = P(("batch", "row"), "col")

    def per_device(lower_tri, right_side, grad_out):
        rows, cols = lower_tri.shape
        width = right_side.shape[1]
        ch = 2 * BLK
        nq, nb = rows // ch, cols // BLK
        nt = sum(nq - b for b in range(NSUM, nb))
        ntot = sum(nq - b for b in range(nb))
        yrows = rows - NSUM * ch
        sd = jax.ShapeDtypeStruct
        n_early = sum(nq - b for b in range(LATE))
        n_late = sum(nq - b for b in range(LATE, nb))
        outs = (sd((rows, width), BF), sd((n_early, ch, BLK), BF), sd((nc, rows, width), BF), sd((nb, nc, BLK, width), BF),
                sd((nr, yrows, width), BF), sd((2, nr, nt, BLK, ch), BF),
                sd((nc, NSUM * BLK - SUM_UP, width), F32), sd((nc, SUM_UP, width), F32))
        vm = pltpu.VMEM
        dma = pltpu.SemaphoreType.DMA
        scratch = [vm((L_BUF, ch, BLK), BF), vm((nt, BLK, ch), BF), vm((NSUM * BLK, rows), BF), vm((2, rows, width), BF), vm((nc, NSUM * BLK, width), F32),
                   vm((NSUM * BLK - SUM_UP, width), F32), vm((SUM_UP, width), F32), vm((nc, NSUM * BLK, width), BF),
                   vm((nr, yrows, width), BF), vm((2, ch, (nq - NSUM) * ch), BF), vm((ch, width), F32), vm((2, ch, width), BF),
                   vm((2, ch, nc * width), BF), vm((2, BLK, nc * width), BF), vm((ch, BLK), F32), vm((2, ch, BLK), BF),
                   dma((14,)), dma((nc, 2)), dma((nb, 2)), dma((nb, nc)), dma((nb * B_CUT, 2)), dma((nb * B_CUT, 2)),
                   dma((6,)), dma((nr, 2)), dma((L_CUT,)), dma((nr * L_CUT, 2, 3)), dma((2, nr, L_CUT)),
                   dma((nc, 2)), dma((nc, 2)), dma((nc, NSUM)), dma((2 * NSUM,)),
                   dma((2, nr, 2)), dma((L_BUF,)), dma((2,)), dma((2,)), dma((nr,)), dma((2, 2, nq - NSUM)), dma((2,)), dma((2, nc)), dma((2, nc)),
                   dma((2,)), dma((nb,))]
        res = pl.pallas_call(
            functools.partial(_kernel, nr, nc),
            out_shape=outs,
            in_specs=[pl.BlockSpec(memory_space=pl.ANY)] * 3,
            out_specs=tuple(pl.BlockSpec(memory_space=pl.ANY) for _ in outs),
            scratch_shapes=scratch,
            compiler_params=pltpu.CompilerParams(collective_id=0, has_side_effects=True, vmem_limit_bytes=VMEM_BYTES),
            name="tri_backward",
        )(lower_tri, right_side, grad_out)
        db, tiles, dxg, bc = res[:4]
        far = nq - LATE
        return pl.pallas_call(
            functools.partial(_last_kernel, nr, nc),
            out_shape=(sd((rows, width), BF), sd((rows, cols), BF)),
            in_specs=[pl.BlockSpec(memory_space=pl.ANY)] * 5,
            out_specs=(pl.BlockSpec(memory_space=pl.ANY),) * 2,
            scratch_shapes=[vm((far, ch, nc * width), BF), vm((far, BLK, nc * width), BF), vm((n_early, ch, BLK), BF), vm((rows, width), BF),
                            vm((ch, BLK), F32), vm((n_late, ch, BLK), BF), vm((ch, BLK), BF),
                            dma((far, nc)), dma((far, nc)), dma((n_early,)), dma((n_early,)), dma((n_late,)),
                            dma((nb * (nb - 1) // 2,)), dma((2,))],
            compiler_params=pltpu.CompilerParams(vmem_limit_bytes=VMEM_BYTES),
            name="tri_backward_last",
        )(grad_out, dxg, bc, tiles, db)

    return jax.shard_map(per_device, mesh=mesh, in_specs=(spec, spec, spec), out_specs=(spec, spec), check_vma=False)
```

```python
import functools
import itertools

import jax
import jax.numpy as jnp
from jax import lax
from jax.experimental import pallas as pl
from jax.experimental.pallas import tpu as pltpu
from jax.sharding import PartitionSpec as P

BLK = 256
NSUM = 3
VMEM_BYTES = 67043328
BF = jnp.bfloat16
F32 = jnp.float32

LATE = 4
B_CUT = 4
L_CUT = 3
SUM_CUT = 2
L_BUF = 4
DX_SEND = 17
DX_EVENTS = (17, 34, 32, 52, 59, 73)
SUM_X = (10, 11, 35, 36, 53, 54, 77, 85)
SUM_LINES = ((29, 20, 4), (45, 20, 4), (52, 20, 4), (65, 20, 4))
BX_LINE = (6, 31, 4)
B_LINES = ((24, 15, 4), (35, 16, 4), (72, 11, 4), (81, 10, 4))
L_LINES = ((43, 4, 4), (87, 11, 4), (92, 12, 4), (98, 11, 4))
Y_EVENTS = (12, 12, 21, 50, 51, 63, 64)
T2_A = 119
T3_A = 92
JA, JC, SUM_UP = 3, 5, 128


def _line(line, n):
    first, num, den = line
    return tuple(first + i * num // den for i in range(n))


def _round_lower(acc, out, b, q, row, col):
    part = BLK // 2
    for i in range(acc.shape[0] // part):
        pos = lax.broadcasted_iota(jnp.int32, (part, BLK), 0) + i * part
        rg = ((2 * q + i * part // BLK) * row[1] + row[0]) * BLK + pos % BLK
        cg = (b * col[1] + col[0]) * BLK + lax.broadcasted_iota(jnp.int32, (part, BLK), 1)
        out[pl.ds(i * part, part)] = jnp.where(rg >= cg, acc[pl.ds(i * part, part)], 0.0).astype(BF)


def _last_kernel(nr, nc, x_ref, dxg, bc, tiles_in, db_in, db_ref, dl_ref, xt, bt, tiles, dbv, acc, made, zero,
                 s_x, s_b, s_in, s_out, s_made, s_zero, s_db):
    rows, cols = dl_ref.shape
    width = x_ref.shape[1]
    ch = 2 * BLK
    nq, nb = rows // ch, cols // BLK
    r = lax.axis_index("row")
    c = lax.axis_index("col")
    early = [(b, q) for b in range(LATE) for q in range(b, nq)]
    late = [(b, q) for q in range(LATE, nq) for b in range(LATE, min(q + 1, nb))]
    above = [(b, q) for b in range(nb) for q in range(b)]

    def place(b, q):
        return dl_ref.at[pl.ds(pl.multiple_of(q * ch, ch), ch), pl.ds(pl.multiple_of(b * BLK, BLK), BLK)]

    def x_load(q, o):
        j = lax.rem(c + o, nc)
        rws = pl.ds(pl.multiple_of((LATE + q) * ch, ch), ch)
        src = x_ref.at[rws] if o == 0 else dxg.at[j, rws]
        return pltpu.make_async_copy(src, xt.at[q, :, pl.ds(pl.multiple_of(j * width, width), width)], s_x.at[q, o])

    def b_load(b, j):
        return pltpu.make_async_copy(bc.at[LATE + b, j], bt.at[b, :, pl.ds(j * width, width)], s_b.at[b, j])

    def tile_load(n):
        return pltpu.make_async_copy(tiles_in.at[n], tiles.at[n], s_in.at[n])

    def tile_store(n):
        return pltpu.make_async_copy(tiles.at[n], place(*early[n]), s_out.at[n])

    def zero_store(n):
        return pltpu.make_async_copy(zero, place(*above[n]), s_zero.at[n])

    db_load = pltpu.make_async_copy(db_in, dbv, s_db.at[0])
    db_store = pltpu.make_async_copy(dbv, db_ref, s_db.at[1])
    for i in range(nq - LATE):
        for o in range(nc):
            x_load(i, o).start()
        for j in range(nc):
            b_load(i, j).start()
    for n in range(len(early)):
        tile_load(n).start()
    db_load.start()
    zero[...] = jnp.zeros_like(zero)
    for n in range(len(above)):
        zero_store(n).start()

    def of(n, vals):
        v = jnp.int32(vals[0])
        for i in range(1, len(vals)):
            v = jnp.where(n >= i, vals[i], v)
        return v

    def made_store(n):
        return pltpu.make_async_copy(made.at[n], place(of(n, [b for b, _ in late]), of(n, [q for _, q in late])), s_made.at[n])

    @pl.loop(0, len(late))
    def _(n):
        b = of(n, [b for b, _ in late])
        q = of(n, [q for _, q in late])

        @pl.when(b == LATE)
        def _():
            for o in range(nc):
                x_load(q - LATE, o).wait()

        @pl.when(b == q)
        def _():
            for j in range(nc):
                b_load(b - LATE, j).wait()

        acc[...] = lax.dot_general(xt[q - LATE], bt[b - LATE], (((1,), (1,)), ((), ())), preferred_element_type=F32)
        _round_lower(acc, made.at[n], b, q, (r, nr), (c, nc))
        made_store(n).start()

        @pl.when(n == len(late) // 2)
        def _():
            for i in range(len(early)):
                tile_load(i).wait()
                tile_store(i).start()
            db_load.wait()
            db_store.start()

    for n in range(len(late)):
        made_store(n).wait()
    for n in range(len(early)):
        tile_store(n).wait()
    for n in range(len(above)):
        zero_store(n).wait()
    db_store.wait()


def _kernel(nr, nc, l_ref, b_ref, x_ref, db_ref, dl_ref, dxg, bc, dxt, ltg, prm, prp,
            lt_in, ltv, lth, dxv, pv, rbm, rbp, sv, dxtv, ltb, acc2, o2, dt, bv, acc3, o3,
            dxs, dxr, bxs, bxr, bys, byr, dys, dyr, lys, lts, ltr, prs, prr, dbs, dbr,
            s_ltz, s_lin, s_dxv, s_rb, s_dxt, s_ltb, s_o2, s_dt, s_bv, s_o3, s_own):
    rows, cols = l_ref.shape
    width = x_ref.shape[1]
    ch = 2 * BLK
    nq = rows // ch
    nb = cols // BLK
    tail = [(b, b) for b in range(NSUM, nb)] + [(b, q) for b in range(NSUM, nb) for q in range(b + 1, nq)]
    ndiag = nb - NSUM
    head = [(b, q) for b in range(NSUM) for q in range(b, nq)]
    nt = len(tail)
    off = {}
    for n, (b, q) in enumerate(tail + head):
        off.setdefault(b, n)
    half = rows // 2
    yrow0 = NSUM * ch
    yhalf = (rows - yrow0) // 2
    cuts = [n for n in range(nt) if n in (0, ndiag) or tail[n - 1][0] != tail[n][0] and n > ndiag][:L_CUT] + [nt]

    nv = nb * B_CUT
    ne = nr * L_CUT
    load_x_at = tuple(max(x - 1, 0) for x in SUM_X)
    sum_at = tuple(_line(x, nc * SUM_CUT) for x in SUM_LINES)
    bx_at = _line(BX_LINE, nb)
    b_slot = tuple(_line(x, nv) for x in B_LINES)
    l_slot = tuple(_line(x, ne) for x in L_LINES)

    z = lax.axis_index("batch")
    r = lax.axis_index("row")
    c = lax.axis_index("col")

    def dev(row, col):
        return (z, row, col)

    def remote(src, dst, ss, rs, to):
        return pltpu.make_async_remote_copy(src, dst, ss, rs, device_id=to, device_id_type=pl.DeviceIdType.MESH)

    def arrived(dst, sem):
        pltpu.make_async_copy(dst, dst, sem).wait()

    def mod(v, m):
        return lax.rem(v + 4 * m, m)

    par = lax.rem(c, 2)
    eps = 1 - 2 * par
    sib = c + eps
    far = mod(c + 4, nc)
    first = mod(c - 2 * eps, nc)
    second = mod(c + 2 * eps, nc)
    hf = par
    hs = 1 - par
    t = lax.rem(c, nr)
    sg = 1 - 2 * lax.rem(t, 2)
    d = mod((r - t) * sg, nr)
    is_root = d == 0
    qc = c // nr

    def row_of(dd):
        return mod(t + sg * dd, nr)

    def piece(o):
        vals = (0, 1, -2, 3, 2, -1, 4, 5)
        v = jnp.int32(vals[0])
        for i in range(1, 8):
            v = jnp.where(o == i, vals[i], v)
        return mod(c + eps * v, nc)

    def table(n, vals):
        v = jnp.int32(vals[0])
        for i in range(1, len(vals)):
            if vals[i] != vals[i - 1]:
                v = jnp.where(n >= i, vals[i], v)
        return v

    def summed(u):
        if isinstance(u, int):
            return u % (nc - 1) + 1 if u else 0
        return jnp.where(u == 0, 0, lax.rem(u, nc - 1) + 1)

    def block_of(n, order):
        return table(n, [b for b, _ in order]), table(n, [q for _, q in order])

    bar = pltpu.get_barrier_semaphore()
    for k in range(1, nc):
        pl.semaphore_signal(bar, inc=1, device_id=dev(r, mod(c + k, nc)), device_id_type=pl.DeviceIdType.MESH)
    for k in range(1, nr):
        pl.semaphore_signal(bar, inc=1, device_id=dev(mod(r + k, nr), c), device_id_type=pl.DeviceIdType.MESH)
    pl.semaphore_wait(bar, nc + nr - 2)

    sends = []

    def note(cond, make, grid=None):
        sends.append((cond, make, grid))

    def bx(b, q):
        src = b_ref.at[pl.ds((2 * b + q) * BLK, BLK)]
        return remote(src, bc.at[b, c], bxs.at[b, q], bxr.at[b, c], dev(r, r + nr * q))

    def bx_start(b):
        for q in range(2):
            @pl.when(c != r + nr * q)
            def _():
                bx(b, q).start()

    for b in range(nb):
        for q in range(2):
            note(c != r + nr * q, functools.partial(bx, b, q))

    def dx_own(h, to, i):
        src = x_ref.at[pl.ds(h * half, half)]
        return remote(src, dxg.at[c, pl.ds(h * half, half)], dxs.at[i], dxr.at[c, h], dev(r, to))

    def dx_fwd(p, h, to, i):
        ref = dxg.at[p, pl.ds(h * half, half)]
        return remote(ref, ref, dxs.at[i], dxr.at[p, h], dev(r, to))

    def dx_wait(p, h):
        arrived(dxg.at[p, pl.ds(h * half, half)], dxr.at[p, h])

    dx_id = itertools.count()
    own_list = [functools.partial(dx_own, hf, second, next(dx_id)), functools.partial(dx_own, hf, sib, next(dx_id)),
                functools.partial(dx_own, hs, second, next(dx_id)), functools.partial(dx_own, hs, sib, next(dx_id)),
                functools.partial(dx_own, hs, first, next(dx_id)), functools.partial(dx_own, hf, first, next(dx_id))]
    ev = [(first, hf, [functools.partial(dx_fwd, first, hf, second, next(dx_id)), functools.partial(dx_fwd, first, hf, sib, next(dx_id))]),
          (first, hs, [functools.partial(dx_fwd, first, hs, sib, next(dx_id))]),
          (second, hs, [functools.partial(dx_fwd, second, hs, first, next(dx_id)), functools.partial(dx_fwd, second, hs, sib, next(dx_id))]),
          (second, hf, [functools.partial(dx_fwd, second, hf, sib, next(dx_id))]),
          (far, hf, [functools.partial(dx_fwd, far, hf, sib, next(dx_id))]),
          (far, hs, [functools.partial(dx_fwd, far, hs, sib, next(dx_id))])]
    for m in own_list:
        note(None, m)
    for _, _, ms in ev:
        for m in ms:
            note(None, m)

    up = mod(r + 1, nr)
    down = mod(r + nr - 1, nr)
    opp = mod(r + 2, nr)

    def dy_own(h, to, i):
        src = x_ref.at[pl.ds(yrow0 + h * yhalf, yhalf)]
        return remote(src, dxt.at[r, pl.ds(h * yhalf, yhalf)], dys.at[i], dyr.at[r, h], dev(to, c))

    def dy_fwd(p, h, to, i):
        ref = dxt.at[p, pl.ds(h * yhalf, yhalf)]
        return remote(ref, ref, dys.at[i], dyr.at[p, h], dev(to, c))

    def dy_wait(p, h):
        arrived(dxt.at[p, pl.ds(h * yhalf, yhalf)], dyr.at[p, h])

    dy_id = itertools.count()
    dy_list = [functools.partial(dy_own, 0, up, next(dy_id)), functools.partial(dy_own, 1, down, next(dy_id)),
               functools.partial(dy_own, 1, up, next(dy_id)), functools.partial(dy_own, 0, down, next(dy_id)),
               functools.partial(dy_fwd, down, 0, up, next(dy_id)), functools.partial(dy_fwd, up, 1, down, next(dy_id))]
    for m in dy_list:
        note(None, m)

    own_list[0]().start()
    own_list[1]().start()
    bx_start(0)
    own_list[2]().start()
    own_list[3]().start()
    dy_list[0]().start()
    dy_list[1]().start()

    def load_x(o, slot):
        return pltpu.make_async_copy(x_ref, dxv.at[slot], s_dxv.at[slot])

    load_x(0, 0).start()

    def own_b(b):
        return pltpu.make_async_copy(b_ref.at[pl.ds((2 * b + qc) * BLK, BLK)], sv.at[summed(b), pl.ds(0, BLK)], s_own.at[b])

    def own_b_out(b):
        return pltpu.make_async_copy(sv.at[summed(b), pl.ds(0, BLK)], bc.at[b, c], bxr.at[b, c])

    @pl.when(is_root)
    def _():
        for b in range(nb):
            own_b(b).start()

    order = tail + head
    ntot = len(order)

    def lin(n):
        b, q = block_of(n, order)
        src = l_ref.at[pl.ds(pl.multiple_of(q * ch, ch), ch), pl.ds(pl.multiple_of(b * BLK, BLK), BLK)]
        return pltpu.make_async_copy(src, lt_in.at[lax.rem(n, L_BUF)], s_lin.at[lax.rem(n, L_BUF)])

    def part_of(ref, i, full):
        n = cuts[i + 1] - cuts[i]
        return ref.at[pl.ds(cuts[i], n)] if full else ref.at[pl.ds(cuts[i], n), :, pl.ds(BLK, BLK)]

    def level(home, src_row, q, i):
        return jnp.where(src_row >= home, 2, 1) - q if i == 0 else jnp.int32(2)

    def by_level(i, lvl, fn):
        @pl.when(lvl == 2)
        def _():
            fn(True)

        if i == 0:
            @pl.when(lvl == 1)
            def _():
                fn(False)

    def ly(i, full):
        return remote(part_of(ltv, i, full), part_of(ltg.at[qc, r], i, full), lys.at[i], ltr.at[qc, r, i], dev(t, c))

    def ly_do(i, op):
        @pl.when(d != 0)
        def _():
            by_level(i, level(t, r, qc, i), lambda full: op(ly(i, full)))

    def l_own(i):
        return pltpu.make_async_copy(part_of(ltv, i, True), part_of(ltg.at[qc, r], i, True), ltr.at[qc, r, i])

    def l_zero(q, rr, j):
        src = lt_in.at[pl.ds(0, ndiag), pl.ds(0, BLK)]
        return pltpu.make_async_copy(src, ltg.at[q, rr, pl.ds(0, ndiag), :, pl.ds(j * BLK, BLK)], s_ltz.at[q, rr, j])

    def l_zeros(op):
        @pl.loop(0, nr)
        def _(rr):
            for q in range(2):
                lvl = level(r, rr, q, 0)
                mine = jnp.logical_and(is_root, jnp.logical_and(rr == r, qc == q))
                for j in range(2):
                    @pl.when(jnp.logical_and(lvl < 2 - j, jnp.logical_not(mine)))
                    def _():
                        op(l_zero(q, rr, j))

    for n in range(L_BUF - 1):
        lin(n).start()
    for b in range(1, NSUM):
        lth[pl.ds(b * BLK, BLK), pl.ds(0, b * ch)] = jnp.zeros((BLK, b * ch), BF)

    @pl.loop(0, ntot)
    def _(n):
        lin(n).wait()

        @pl.when(n + L_BUF - 1 < ntot)
        def _():
            lin(n + L_BUF - 1).start()

        blk = lt_in[lax.rem(n, L_BUF)].T

        @pl.when(n < nt)
        def _():
            ltv[n] = blk

        @pl.when(n >= nt)
        def _():
            b, q = block_of(n, order)
            lth[pl.ds(pl.multiple_of(b * BLK, BLK), BLK), pl.ds(pl.multiple_of(q * ch, ch), ch)] = blk

        for i in range(L_CUT):
            @pl.when(n == cuts[i + 1] - 1)
            def _():
                @pl.when(is_root)
                def _():
                    l_own(i).start()

                ly_do(i, lambda cp: cp.start())

    lt_in[...] = jnp.zeros_like(lt_in)
    l_zeros(lambda cp: cp.start())

    @pl.when(is_root)
    def _():
        for b in range(nb):
            own_b(b).wait()
        for b in range(nb):
            own_b_out(b).start()

    on_ring = par == lax.rem(r, 2)

    def l_do(q, e, w, to, op):
        rr = mod(r + lax.rem(e, nr), nr)

        def go(i, full):
            ref = part_of(ltg.at[q, rr], i, full)
            op(remote(ref, ref, lts.at[e, q, w], ltr.at[q, rr, i], dev(r, to)))

        for i in range(L_CUT):
            @pl.when(e // nr == i)
            def _():
                by_level(i, level(r, rr, q, i), functools.partial(go, i))

    def l_send(q, e, w, to):
        l_do(q, e, w, to, lambda cp: cp.start())

    def l_wait(q, e):
        rr = mod(r + lax.rem(e, nr), nr)
        mine = jnp.logical_and(is_root, jnp.logical_and(rr == r, qc == q))

        def go(i, full):
            arrived(part_of(ltg.at[q, rr], i, full), ltr.at[q, rr, i])

        for i in range(L_CUT):
            @pl.when(e // nr == i)
            def _():
                by_level(i, jnp.where(mine, 2, level(r, rr, q, i)), functools.partial(go, i))

    right = mod(c + 2, nc)
    left = mod(c - 2, nc)
    def l_fwd(q, e, op):
        side = lax.rem(e, nr) // 2
        from_left = c == mod(r + nr * q + 2, nc)

        @pl.when(from_left == (side == 0))
        def _():
            l_do(q, e, 0, jnp.where(from_left, right, left), op)

    def l_stage0(e):
        l_wait(qc, e)
        l_send(qc, e, 0, right)
        l_send(qc, e, 1, left)
        l_send(qc, e, 2, sib)

    def l_stage1(e):
        for q in range(2):
            l_wait(q, e)
            l_fwd(q, e, lambda cp: cp.start())
            l_send(q, e, 2, sib)

    def l_stage2(e):
        l_wait(1 - qc, e)
        l_send(1 - qc, e, 2, sib)

    def l_stage3(e):
        for q in range(2):
            l_wait(q, e)

    bh = BLK // B_CUT

    def b_ref_of(v, lo, hi):
        return bc.at[v // B_CUT, pl.ds(lo, hi - lo), pl.ds(lax.rem(v, B_CUT) * bh, bh)]

    def b_send(v, lo, hi, ss, rs, dd):
        ref = b_ref_of(v, lo, hi)
        return remote(ref, ref, bys.at[v, ss], byr.at[v, rs], dev(row_of(dd), c))

    def b_wait(v, lo, hi, rs):
        arrived(b_ref_of(v, lo, hi), byr.at[v, rs])

    ja, jc = JA, JC
    b_moves = [(0, lambda v: b_send(v, 0, nc, 0, 0, 3)), (0, lambda v: b_send(v, ja, nc, 1, 0, 1)),
               (3, lambda v: b_send(v, 0, jc, 0, 0, 2)), (1, lambda v: b_send(v, jc, nc, 0, 1, 2)),
               (2, lambda v: b_send(v, 0, ja, 0, 1, 1))]

    mrow = SUM_UP
    prows = NSUM * BLK
    hrow = (prows - mrow) // SUM_CUT

    def sum_parts(o, i):
        if i is None:
            return pv.at[o, pl.ds(0, mrow)], prp.at[o], rbp, SUM_CUT
        return pv.at[o, pl.ds(pl.multiple_of(mrow + i * hrow, 16), hrow)], prm.at[o, i], rbm, i

    def sum_send(o, i):
        src, dst, _, k = sum_parts(o, i)
        to = row_of(mod(d + (1 if i is None else -1), nr))
        return remote(src, dst, prs.at[o, k], prr.at[o, k], dev(to, c))

    def sum_step(o, i):
        own, land, buf, k = sum_parts(o, i)
        arrived(land, prr.at[o, k])
        cp = pltpu.make_async_copy(land, buf, s_rb.at[0 if i is None else 1])
        cp.start()
        cp.wait()

        @pl.loop(0, buf.shape[0] // 16)
        def _(j):
            own[pl.ds(j * 16, 16)] = own[pl.ds(j * 16, 16)] + buf[pl.ds(j * 16, 16)]

        @pl.when(jnp.logical_not(is_root))
        def _():
            sum_send(o, i).start()

    def out_send(o, b, to):
        dst = db_ref.at[pl.ds((2 * b + qc) * BLK, BLK)]
        return remote(sv.at[o, pl.ds(b * BLK, BLK)], dst, dbs.at[o, b], dbr.at[2 * b + qc], dev(r, to))

    def out_local(o, b):
        dst = db_ref.at[pl.ds((2 * b + qc) * BLK, BLK)]
        return pltpu.make_async_copy(sv.at[o, pl.ds(b * BLK, BLK)], dst, dbr.at[2 * b + qc])

    def finish(o):
        @pl.loop(0, prows // 64)
        def _(i):
            sv[o, pl.ds(i * 64, 64)] = pv[o, pl.ds(i * 64, 64)].astype(BF)

        for b in range(NSUM):
            @pl.when(o == 0)
            def _():
                out_local(o, b).start()

            @pl.when(o != 0)
            def _():
                out_send(o, b, piece(o)).start()

    def partial(o):
        pv[o] = jnp.dot(lth[...], dxv[lax.rem(o, 2)], preferred_element_type=F32)

    offd = [next((n for n, x in enumerate(tail) if n >= ndiag and x[0] == b), nt) for b in range(NSUM, nb)]
    n2 = (nb - NSUM) * nr

    def t2_load(w, q, i):
        g, k = w // nr, lax.rem(w, 2)
        n = jnp.where(i == 0, g, table(g, offd) + i - 1)
        dst = ltb.at[k, pl.ds(q * BLK, BLK), pl.ds(pl.multiple_of(i * ch, ch), ch)]
        return pltpu.make_async_copy(ltg.at[q, lax.rem(w, nr), n], dst, s_ltb.at[k, q, i])

    def t2_loads(w, op):
        @pl.loop(0, nq - NSUM - w // nr)
        def _(i):
            for q in range(2):
                op(t2_load(w, q, i))

    def t2_start(w):
        t2_loads(w, lambda cp: cp.start())

    def t2_out(g):
        k = lax.rem(g, 2)
        return pltpu.make_async_copy(o2.at[k], db_ref.at[pl.ds((NSUM + g) * ch, ch)], s_o2.at[k])

    def t2_item(w):
        g, rr, k = w // nr, lax.rem(w, nr), lax.rem(w, 2)
        t2_loads(w, lambda cp: cp.wait())

        @pl.when(w + 1 < n2)
        def _():
            t2_start(w + 1)

        for gg in range(nb - NSUM):
            @pl.when(g == gg)
            def _():
                deep = (nq - NSUM - gg) * ch
                v = jnp.dot(ltb[k, :, pl.ds(0, deep)], dxtv[rr, pl.ds(gg * ch, deep)], preferred_element_type=F32)

                @pl.when(rr == 0)
                def _():
                    acc2[...] = v

                @pl.when(rr != 0)
                def _():
                    acc2[...] = acc2[...] + v

        @pl.when(rr == nr - 1)
        def _():
            @pl.when(g >= 2)
            def _():
                t2_out(g - 2).wait()
            o2[lax.rem(g, 2)] = acc2[...].astype(BF)
            t2_out(g).start()

    t3_order = [(b, q) for b in range(LATE) for q in range(b, nq)]
    n3 = len(t3_order)
    t3_last = [max(n for n, (bb, _) in enumerate(t3_order) if bb == b) for b in range(LATE)]

    def t3_load(n, o):
        b, q = block_of(n, t3_order)
        k = lax.rem(n, 2)
        rws = pl.ds(pl.multiple_of(q * ch, ch), ch)
        src = x_ref.at[rws] if o == 0 else dxg.at[mod(c + o, nc), rws]
        return pltpu.make_async_copy(src, dt.at[k, :, pl.ds(pl.multiple_of(mod(c + o, nc) * width, width), width)], s_dt.at[k, o])

    def bv_load(b, j):
        k = lax.rem(b, 2)
        return pltpu.make_async_copy(bc.at[b, j], bv.at[k, :, pl.ds(j * width, width)], s_bv.at[k, j])

    def t3_out(n):
        k = lax.rem(n, 2)
        return pltpu.make_async_copy(o3.at[k], dl_ref.at[n], s_o3.at[k])

    def t3_item(n):
        b, q = block_of(n, t3_order)
        k = lax.rem(n, 2)
        for o in range(nc):
            t3_load(n, o).wait()

        @pl.when(n + 1 < n3)
        def _():
            for o in range(nc):
                t3_load(n + 1, o).start()

        @pl.when(q == b)
        def _():
            for j in range(nc):
                bv_load(b, j).wait()

        acc3[...] = lax.dot_general(dt[k], bv[lax.rem(b, 2)], (((1,), (1,)), ((), ())), preferred_element_type=F32)

        @pl.when(n >= 2)
        def _():
            t3_out(n - 2).wait()

        _round_lower(acc3, o3.at[k], b, q, (r, nr), (c, nc))
        t3_out(n).start()
    b_ready = [max(x[B_CUT * b + B_CUT - 1] for x in b_slot) for b in range(nb)]
    l_ready = [max(x[nr * i + nr - 1] for x in l_slot) for i in range(L_CUT)]
    t2_need = [l_ready[min(w // nr + 1, L_CUT - 1)] for w in range(n2)]

    def packed(start, ready):
        out = []
        for n in range(len(ready)):
            out.append(max(start, ready[n], out[-1] + 1 if out else 0))
        return out

    t2_slots = packed(T2_A, t2_need[1:] + t2_need[-1:])
    t3_slots, bv_slots = [], []
    for b in range(LATE):
        bv_slots.append(max(b_ready[b], T3_A - 1 if b < 2 else t3_slots[t3_last[b - 2]]))
        t3_slots = packed(T3_A, t3_slots + [bv_slots[b] + 1] * (nq - b))
    assert T2_A > max(l_ready[1], Y_EVENTS[6]) and Y_EVENTS[6] > max(Y_EVENTS[3:6])
    assert T3_A > max(load_x_at[-1], DX_EVENTS[-1])
    lists = (sum_at, b_slot, l_slot)
    assert all(a < b for f in lists + ((SUM_X,),) for x in f for a, b in zip(x[:-1], x[1:]))
    assert all(sum_at[0][u * SUM_CUT] > SUM_X[summed(u)] for u in range(nc))
    assert all(a < b for f in lists for y, z in zip(f[:-1], f[1:]) for a, b in zip(y, z))
    assert all(SUM_X[o - 2] < load_x_at[o] for o in range(2, nc))
    assert all(max(DX_EVENTS[o:o + 2]) <= load_x_at[o + 2] for o in (0, 2, 4))
    assert all(b_slot[0][B_CUT * b] <= sum_at[-1][b * SUM_CUT + SUM_CUT - 1] for b in range(nb))
    slots = 1 + max(t3_slots[-1], t2_slots[-1], sum_at[-1][-1], b_ready[-1], l_ready[-1])

    down_depth = nr - 1 - d
    up_depth = mod(d - 1, nr)
    off_ring = jnp.logical_not(on_ring)

    def listed(vals):
        return lambda n: table(n, tuple(vals) + (slots,))

    events = []

    def event(slot, fn):
        events.append((slot, fn))

    def dx_event(i):
        p, h, ms = ev[i]
        dx_wait(p, h)
        for m in ms:
            m().start()

    def dx_rest():
        for m in own_list[4:]:
            m().start()

    def bx_event(b):
        bx_start(b)

    def y_first():
        dy_list[2]().start()
        dy_list[3]().start()

    def y_event(i):
        if i == 1:
            dy_wait(down, 0)
            dy_list[4]().start()
        elif i == 2:
            dy_wait(up, 1)
            dy_list[5]().start()
        elif i == 3:
            dy_wait(down, 1)
        elif i == 4:
            dy_wait(up, 0)
        else:
            dy_wait(opp, 0)
            dy_wait(opp, 1)

    def y_load(op):
        for i in range(nr):
            rr = mod(r + i, nr)
            src = x_ref.at[pl.ds(yrow0, 2 * yhalf)] if i == 0 else dxt.at[rr]
            op(pltpu.make_async_copy(src, dxtv.at[rr], s_dxt.at[i]))

    def t2_first():
        l_zeros(lambda cp: cp.wait())
        t2_start(0)
        y_load(lambda cp: cp.wait())

    def t3_first():
        for o in range(nc):
            t3_load(0, o).start()

    def bv_event(b):
        for j in range(nc):
            bv_load(b, j).start()

    for i in range(len(ev)):
        event(DX_EVENTS[i], functools.partial(dx_event, i))
    event(DX_SEND, dx_rest)
    for b in range(1, nb):
        event(bx_at[b], functools.partial(bx_event, b))
    event(Y_EVENTS[0], y_first)
    for i in range(1, 6):
        event(Y_EVENTS[i], functools.partial(y_event, i))
    event(Y_EVENTS[6], lambda: y_load(lambda cp: cp.start()))
    n_first = len(events)
    event(T2_A - 1, t2_first)
    event(T3_A - 1, t3_first)
    for b in range(LATE):
        event(bv_slots[b], functools.partial(bv_event, b))

    def event_flow(lo, hi):
        part = sorted(range(lo, hi), key=lambda i: events[i][0])
        at = sorted({events[i][0] for i in part})
        masks = [sum(1 << (i - lo) for i in part if events[i][0] == x) for x in at]

        def run(k):
            mask = table(k, masks)
            for i in range(lo, hi):
                @pl.when(jnp.bitwise_and(mask, 1 << (i - lo)) != 0)
                def _():
                    events[i][1]()

        return listed(at), len(at), run

    def b_due(v):
        @pl.when(is_root)
        def _():
            @pl.when(lax.rem(v, B_CUT) == 0)
            def _():
                @pl.loop(0, nc)
                def _(j):
                    arrived(bc.at[v // B_CUT, j], bxr.at[v // B_CUT, j])
            b_moves[0][1](v).start()
            b_moves[1][1](v).start()

        @pl.when(d == 3)
        def _():
            b_wait(v, 0, nc, 0)
            b_moves[2][1](v).start()

        @pl.when(d == 1)
        def _():
            b_wait(v, ja, nc, 0)
            b_moves[3][1](v).start()

        @pl.when(d == 2)
        def _():
            b_wait(v, 0, jc, 0)
            b_moves[4][1](v).start()
            b_wait(v, jc, nc, 1)

    def b_last(v):
        b_wait(v, 0, ja, 1)

    def l_due(e):
        @pl.when(is_root)
        def _():
            l_stage0(e)

        @pl.when(off_ring)
        def _():
            l_stage3(e)

        @pl.when(jnp.logical_and(on_ring, jnp.logical_not(is_root)))
        def _():
            l_stage1(e)

    def sum_due(o, i, depth):
        @pl.when(depth == 0)
        def _():
            sum_send(o, i).start()

        @pl.when(depth > 0)
        def _():
            sum_step(o, i)

    def down_due(n):
        sum_due(summed(n // SUM_CUT), lax.rem(n, SUM_CUT), down_depth)

    def load_due(o):
        p = piece(o)
        k = lax.rem(o, 2)

        @pl.when(k == 1)
        def _():
            dx_wait(p, 0)
            dx_wait(p, 1)

        @pl.when(o > 0)
        def _():
            pltpu.make_async_copy(dxg.at[p], dxv.at[k], s_dxv.at[k]).start()

    def part_due(o):
        load_x(0, lax.rem(o, 2)).wait()
        partial(o)

    def stage(lines, k, total):
        first = jnp.int32(slots)
        num = jnp.int32(0)
        for i, (f, m, _) in enumerate(lines):
            first = jnp.where(k == i, f, first)
            num = jnp.where(k == i, m, num)
        return lambda n: jnp.where(n < total, first + n * num // 4, slots)

    def up_due(u):
        sum_due(summed(u), None, up_depth)

        @pl.when(is_root)
        def _():
            finish(summed(u))

    none = jnp.int32(-1)
    flows = [event_flow(0, n_first)[::2],
             (stage(L_LINES, jnp.where(is_root, 0, jnp.where(off_ring, 3, 1)), ne), l_due),
             (stage(L_LINES, jnp.where(is_root, 2, none), ne), l_stage2),
             (stage(B_LINES, jnp.where(d == 0, 0, jnp.where(d == 2, 2, 1)), nv), b_due),
             (stage(B_LINES, jnp.where(d == 1, 3, none), nv), b_last),
             (stage(SUM_LINES, down_depth, nc * SUM_CUT), down_due),
             (lambda n: stage(SUM_LINES, up_depth, nc * SUM_CUT)(n * SUM_CUT + SUM_CUT - 1), up_due),
             (listed(load_x_at), load_due),
             (listed(SUM_X), part_due),
             event_flow(n_first, n_first + 2)[::2],
             (listed(t2_slots), t2_item), (listed(t3_slots), t3_item), event_flow(n_first + 2, len(events))[::2]]

    def slot(s, carry):
        nxt = []
        for (when, fn), (n, at) in zip(flows, carry):
            def go(n, fn=fn, when=when):
                fn(n)
                return n + 1, when(n + 1)

            def stay(n, at=at):
                return n, at

            nxt.append(lax.cond(at == s, go, stay, n))
        return tuple(nxt)

    lax.fori_loop(0, slots, slot, tuple((jnp.int32(0), jnp.int32(when(jnp.int32(0)))) for when, _ in flows))

    for g in (n2 // nr - 2, n2 // nr - 1):
        t2_out(g).wait()
    for n in (n3 - 2, n3 - 1):
        t3_out(n).wait()
    for i in range(2 * NSUM):
        arrived(db_ref.at[pl.ds(i * BLK, BLK)], dbr.at[i])

    for cond, make, _ in sends:
        if cond is None:
            make().wait_send()
        else:
            @pl.when(cond)
            def _():
                make().wait_send()

    @pl.loop(0, nv)
    def _(v):
        for dd, make in b_moves:
            @pl.when(d == dd)
            def _():
                make(v).wait_send()

    def sent(cp):
        cp.wait_send()

    for i in range(L_CUT):
        ly_do(i, sent)

    @pl.loop(0, ne)
    def _(e):
        @pl.when(is_root)
        def _():
            l_do(qc, e, 0, right, sent)
            l_do(qc, e, 1, left, sent)
            l_do(qc, e, 2, sib, sent)
            l_do(1 - qc, e, 2, sib, sent)

        @pl.when(jnp.logical_and(on_ring, jnp.logical_not(is_root)))
        def _():
            for q in range(2):
                l_fwd(q, e, sent)
                l_do(q, e, 2, sib, sent)

    @pl.loop(0, 8)
    def _(o):
        @pl.when(jnp.logical_not(is_root))
        def _():
            for i in (None,) + tuple(range(SUM_CUT)):
                sum_send(o, i).wait_send()

        @pl.when(jnp.logical_and(is_root, o != 0))
        def _():
            for b in range(NSUM):
                out_send(o, b, piece(o)).wait_send()


def solution(mesh):
    nr = mesh.shape["row"]
    nc = mesh.shape["col"]
    spec = P(("batch", "row"), "col")

    def per_device(lower_tri, right_side, grad_out):
        rows, cols = lower_tri.shape
        width = right_side.shape[1]
        ch = 2 * BLK
        nq, nb = rows // ch, cols // BLK
        nt = sum(nq - b for b in range(NSUM, nb))
        ntot = sum(nq - b for b in range(nb))
        yrows = rows - NSUM * ch
        sd = jax.ShapeDtypeStruct
        n_early = sum(nq - b for b in range(LATE))
        n_late = sum(nq - b for b in range(LATE, nb))
        outs = (sd((rows, width), BF), sd((n_early, ch, BLK), BF), sd((nc, rows, width), BF), sd((nb, nc, BLK, width), BF),
                sd((nr, yrows, width), BF), sd((2, nr, nt, BLK, ch), BF),
                sd((nc, SUM_CUT, (NSUM * BLK - SUM_UP) // SUM_CUT, width), F32), sd((nc, SUM_UP, width), F32))
        vm = pltpu.VMEM
        dma = pltpu.SemaphoreType.DMA
        scratch = [vm((L_BUF, ch, BLK), BF), vm((nt, BLK, ch), BF), vm((NSUM * BLK, rows), BF), vm((2, rows, width), BF), vm((nc, NSUM * BLK, width), F32),
                   vm(((NSUM * BLK - SUM_UP) // SUM_CUT, width), F32), vm((SUM_UP, width), F32), vm((nc, NSUM * BLK, width), BF),
                   vm((nr, yrows, width), BF), vm((2, ch, (nq - NSUM) * ch), BF), vm((ch, width), F32), vm((2, ch, width), BF),
                   vm((2, ch, nc * width), BF), vm((2, BLK, nc * width), BF), vm((ch, BLK), F32), vm((2, ch, BLK), BF),
                   dma((14,)), dma((nc, 2)), dma((nb, 2)), dma((nb, nc)), dma((nb * B_CUT, 2)), dma((nb * B_CUT, 2)),
                   dma((6,)), dma((nr, 2)), dma((L_CUT,)), dma((nr * L_CUT, 2, 3)), dma((2, nr, L_CUT)),
                   dma((nc, SUM_CUT + 1)), dma((nc, SUM_CUT + 1)), dma((nc, NSUM)), dma((2 * NSUM,)),
                   dma((2, nr, 2)), dma((L_BUF,)), dma((2,)), dma((2,)), dma((nr,)), dma((2, 2, nq - NSUM)), dma((2,)), dma((2, nc)), dma((2, nc)),
                   dma((2,)), dma((nb,))]
        res = pl.pallas_call(
            functools.partial(_kernel, nr, nc),
            out_shape=outs,
            in_specs=[pl.BlockSpec(memory_space=pl.ANY)] * 3,
            out_specs=tuple(pl.BlockSpec(memory_space=pl.ANY) for _ in outs),
            scratch_shapes=scratch,
            compiler_params=pltpu.CompilerParams(collective_id=0, has_side_effects=True, vmem_limit_bytes=VMEM_BYTES),
            name="tri_backward",
        )(lower_tri, right_side, grad_out)
        db, tiles, dxg, bc = res[:4]
        far = nq - LATE
        return pl.pallas_call(
            functools.partial(_last_kernel, nr, nc),
            out_shape=(sd((rows, width), BF), sd((rows, cols), BF)),
            in_specs=[pl.BlockSpec(memory_space=pl.ANY)] * 5,
            out_specs=(pl.BlockSpec(memory_space=pl.ANY),) * 2,
            scratch_shapes=[vm((far, ch, nc * width), BF), vm((far, BLK, nc * width), BF), vm((n_early, ch, BLK), BF), vm((rows, width), BF),
                            vm((ch, BLK), F32), vm((n_late, ch, BLK), BF), vm((ch, BLK), BF),
                            dma((far, nc)), dma((far, nc)), dma((n_early,)), dma((n_early,)), dma((n_late,)),
                            dma((nb * (nb - 1) // 2,)), dma((2,))],
            compiler_params=pltpu.CompilerParams(vmem_limit_bytes=VMEM_BYTES),
            name="tri_backward_last",
        )(grad_out, dxg, bc, tiles, db)

    return jax.shard_map(per_device, mesh=mesh, in_specs=(spec, spec, spec), out_specs=(spec, spec), check_vma=False)
```

```python
import functools
import itertools

import jax
import jax.numpy as jnp
from jax import lax
from jax.experimental import pallas as pl
from jax.experimental.pallas import tpu as pltpu
from jax.sharding import PartitionSpec as P

BLK = 256
NSUM = 3
VMEM_BYTES = 67043328
BF = jnp.bfloat16
F32 = jnp.float32

LATE = 4
B_CUT = 4
L_CUT = 3
SUM_CUT = 2
L_BUF = 4
DX_SEND = 24
DX_EVENTS = (26, 35, 39, 59, 67, 74)
SUM_X = (12, 13, 36, 37, 60, 61, 79, 80)
SUM_LINES = ((31, 20, 4), (45, 20, 4), (54, 20, 4), (65, 20, 4))
BX_LINE = (8, 31, 4)
B_LINES = ((21, 15, 4), (32, 16, 4), (69, 11, 4), (80, 10, 4))
L_LINES = ((38, 6, 4), (82, 13, 4), (90, 13, 4), (99, 10, 4))
Y_EVENTS = (12, 14, 24, 50, 51, 70, 71)
T2_A = 122
T3_A = 80
JA, JC, SUM_UP = 3, (5, 4), 128


def _line(line, n):
    first, num, den = line
    return tuple(first + i * num // den for i in range(n))


def _round_lower(acc, out, b, q, row, col):
    part = BLK // 2
    for i in range(acc.shape[0] // part):
        pos = lax.broadcasted_iota(jnp.int32, (part, BLK), 0) + i * part
        rg = ((2 * q + i * part // BLK) * row[1] + row[0]) * BLK + pos % BLK
        cg = (b * col[1] + col[0]) * BLK + lax.broadcasted_iota(jnp.int32, (part, BLK), 1)
        out[pl.ds(i * part, part)] = jnp.where(rg >= cg, acc[pl.ds(i * part, part)], 0.0).astype(BF)


def _last_kernel(nr, nc, x_ref, dxg, bc, tiles_in, db_in, db_ref, dl_ref, xt, bt, tiles, dbv, acc, made, zero,
                 s_x, s_b, s_in, s_out, s_made, s_zero, s_db):
    rows, cols = dl_ref.shape
    width = x_ref.shape[1]
    ch = 2 * BLK
    nq, nb = rows // ch, cols // BLK
    r = lax.axis_index("row")
    c = lax.axis_index("col")
    early = [(b, q) for b in range(LATE) for q in range(b, nq)]
    late = [(b, q) for q in range(LATE, nq) for b in range(LATE, min(q + 1, nb))]
    above = [(b, q) for b in range(nb) for q in range(b)]

    def place(b, q):
        return dl_ref.at[pl.ds(pl.multiple_of(q * ch, ch), ch), pl.ds(pl.multiple_of(b * BLK, BLK), BLK)]

    def x_load(q, o):
        j = lax.rem(c + o, nc)
        rws = pl.ds(pl.multiple_of((LATE + q) * ch, ch), ch)
        src = x_ref.at[rws] if o == 0 else dxg.at[j, rws]
        return pltpu.make_async_copy(src, xt.at[q, :, pl.ds(pl.multiple_of(j * width, width), width)], s_x.at[q, o])

    def b_load(b, j):
        return pltpu.make_async_copy(bc.at[LATE + b, j], bt.at[b, :, pl.ds(j * width, width)], s_b.at[b, j])

    def tile_load(n):
        return pltpu.make_async_copy(tiles_in.at[n], tiles.at[n], s_in.at[n])

    def tile_store(n):
        return pltpu.make_async_copy(tiles.at[n], place(*early[n]), s_out.at[n])

    def zero_store(n):
        return pltpu.make_async_copy(zero, place(*above[n]), s_zero.at[n])

    db_load = pltpu.make_async_copy(db_in, dbv, s_db.at[0])
    db_store = pltpu.make_async_copy(dbv, db_ref, s_db.at[1])
    for i in range(nq - LATE):
        for o in range(nc):
            x_load(i, o).start()
        for j in range(nc):
            b_load(i, j).start()
    for n in range(len(early)):
        tile_load(n).start()
    db_load.start()
    zero[...] = jnp.zeros_like(zero)
    for n in range(len(above)):
        zero_store(n).start()

    def of(n, vals):
        v = jnp.int32(vals[0])
        for i in range(1, len(vals)):
            v = jnp.where(n >= i, vals[i], v)
        return v

    def made_store(n):
        return pltpu.make_async_copy(made.at[n], place(of(n, [b for b, _ in late]), of(n, [q for _, q in late])), s_made.at[n])

    @pl.loop(0, len(late))
    def _(n):
        b = of(n, [b for b, _ in late])
        q = of(n, [q for _, q in late])

        @pl.when(b == LATE)
        def _():
            for o in range(nc):
                x_load(q - LATE, o).wait()

        @pl.when(b == q)
        def _():
            for j in range(nc):
                b_load(b - LATE, j).wait()

        acc[...] = lax.dot_general(xt[q - LATE], bt[b - LATE], (((1,), (1,)), ((), ())), preferred_element_type=F32)
        _round_lower(acc, made.at[n], b, q, (r, nr), (c, nc))
        made_store(n).start()

        @pl.when(n == len(late) // 2)
        def _():
            for i in range(len(early)):
                tile_load(i).wait()
                tile_store(i).start()
            db_load.wait()
            db_store.start()

    for n in range(len(late)):
        made_store(n).wait()
    for n in range(len(early)):
        tile_store(n).wait()
    for n in range(len(above)):
        zero_store(n).wait()
    db_store.wait()


def _kernel(nr, nc, l_ref, b_ref, x_ref, db_ref, dl_ref, dxg, bc, dxt, ltg, prm, prp,
            lt_in, ltv, lth, dxv, pv, rbm, rbp, sv, dxtv, ltb, acc2, o2, dt, bv, acc3, o3,
            dxs, dxr, bxs, bxr, bys, byr, dys, dyr, lys, lts, ltr, prs, prr, dbs, dbr,
            s_ltz, s_lin, s_dxv, s_rb, s_dxt, s_ltb, s_o2, s_dt, s_bv, s_o3, s_own):
    rows, cols = l_ref.shape
    width = x_ref.shape[1]
    ch = 2 * BLK
    nq = rows // ch
    nb = cols // BLK
    tail = [(b, b) for b in range(NSUM, nb)] + [(b, q) for b in range(NSUM, nb) for q in range(b + 1, nq)]
    ndiag = nb - NSUM
    head = [(b, q) for b in range(NSUM) for q in range(b, nq)]
    nt = len(tail)
    off = {}
    for n, (b, q) in enumerate(tail + head):
        off.setdefault(b, n)
    half = rows // 2
    yrow0 = NSUM * ch
    yhalf = (rows - yrow0) // 2
    cuts = [n for n in range(nt) if n in (0, ndiag) or tail[n - 1][0] != tail[n][0] and n > ndiag][:L_CUT] + [nt]

    nv = nb * B_CUT
    ne = nr * L_CUT
    load_x_at = tuple(max(x - 1, 0) for x in SUM_X)
    sum_at = tuple(_line(x, nc * SUM_CUT) for x in SUM_LINES)
    bx_at = _line(BX_LINE, nb)
    b_slot = tuple(_line(x, nv) for x in B_LINES)
    l_slot = tuple(_line(x, ne) for x in L_LINES)

    z = lax.axis_index("batch")
    r = lax.axis_index("row")
    c = lax.axis_index("col")

    def dev(row, col):
        return (z, row, col)

    def remote(src, dst, ss, rs, to):
        return pltpu.make_async_remote_copy(src, dst, ss, rs, device_id=to, device_id_type=pl.DeviceIdType.MESH)

    def arrived(dst, sem):
        pltpu.make_async_copy(dst, dst, sem).wait()

    def mod(v, m):
        return lax.rem(v + 4 * m, m)

    par = lax.rem(c, 2)
    eps = 1 - 2 * par
    sib = c + eps
    far = mod(c + 4, nc)
    first = mod(c - 2 * eps, nc)
    second = mod(c + 2 * eps, nc)
    hf = par
    hs = 1 - par
    t = lax.rem(c, nr)
    sg = 1 - 2 * lax.rem(t, 2)
    d = mod((r - t) * sg, nr)
    is_root = d == 0
    qc = c // nr

    def row_of(dd):
        return mod(t + sg * dd, nr)

    def piece(o):
        vals = (0, 1, -2, 3, 2, -1, 4, 5)
        v = jnp.int32(vals[0])
        for i in range(1, 8):
            v = jnp.where(o == i, vals[i], v)
        return mod(c + eps * v, nc)

    def table(n, vals):
        v = jnp.int32(vals[0])
        for i in range(1, len(vals)):
            if vals[i] != vals[i - 1]:
                v = jnp.where(n >= i, vals[i], v)
        return v

    def summed(u):
        if isinstance(u, int):
            return u % (nc - 1) + 1 if u else 0
        return jnp.where(u == 0, 0, lax.rem(u, nc - 1) + 1)

    def block_of(n, order):
        return table(n, [b for b, _ in order]), table(n, [q for _, q in order])

    bar = pltpu.get_barrier_semaphore()
    for k in range(1, nc):
        pl.semaphore_signal(bar, inc=1, device_id=dev(r, mod(c + k, nc)), device_id_type=pl.DeviceIdType.MESH)
    for k in range(1, nr):
        pl.semaphore_signal(bar, inc=1, device_id=dev(mod(r + k, nr), c), device_id_type=pl.DeviceIdType.MESH)
    pl.semaphore_wait(bar, nc + nr - 2)

    sends = []

    def note(cond, make, grid=None):
        sends.append((cond, make, grid))

    def bx(b, q):
        src = b_ref.at[pl.ds((2 * b + q) * BLK, BLK)]
        return remote(src, bc.at[b, c], bxs.at[b, q], bxr.at[b, c], dev(r, r + nr * q))

    def bx_start(b):
        for q in range(2):
            @pl.when(c != r + nr * q)
            def _():
                bx(b, q).start()

    for b in range(nb):
        for q in range(2):
            note(c != r + nr * q, functools.partial(bx, b, q))

    def dx_own(h, to, i):
        src = x_ref.at[pl.ds(h * half, half)]
        return remote(src, dxg.at[c, pl.ds(h * half, half)], dxs.at[i], dxr.at[c, h], dev(r, to))

    def dx_fwd(p, h, to, i):
        ref = dxg.at[p, pl.ds(h * half, half)]
        return remote(ref, ref, dxs.at[i], dxr.at[p, h], dev(r, to))

    def dx_wait(p, h):
        arrived(dxg.at[p, pl.ds(h * half, half)], dxr.at[p, h])

    dx_id = itertools.count()
    own_list = [functools.partial(dx_own, hf, second, next(dx_id)), functools.partial(dx_own, hf, sib, next(dx_id)),
                functools.partial(dx_own, hs, second, next(dx_id)), functools.partial(dx_own, hs, sib, next(dx_id)),
                functools.partial(dx_own, hs, first, next(dx_id)), functools.partial(dx_own, hf, first, next(dx_id))]
    ev = [(first, hf, [functools.partial(dx_fwd, first, hf, second, next(dx_id)), functools.partial(dx_fwd, first, hf, sib, next(dx_id))]),
          (first, hs, [functools.partial(dx_fwd, first, hs, sib, next(dx_id))]),
          (second, hs, [functools.partial(dx_fwd, second, hs, first, next(dx_id)), functools.partial(dx_fwd, second, hs, sib, next(dx_id))]),
          (second, hf, [functools.partial(dx_fwd, second, hf, sib, next(dx_id))]),
          (far, hf, [functools.partial(dx_fwd, far, hf, sib, next(dx_id))]),
          (far, hs, [functools.partial(dx_fwd, far, hs, sib, next(dx_id))])]
    for m in own_list:
        note(None, m)
    for _, _, ms in ev:
        for m in ms:
            note(None, m)

    up = mod(r + 1, nr)
    down = mod(r + nr - 1, nr)
    opp = mod(r + 2, nr)

    def dy_own(h, to, i):
        src = x_ref.at[pl.ds(yrow0 + h * yhalf, yhalf)]
        return remote(src, dxt.at[r, pl.ds(h * yhalf, yhalf)], dys.at[i], dyr.at[r, h], dev(to, c))

    def dy_fwd(p, h, to, i):
        ref = dxt.at[p, pl.ds(h * yhalf, yhalf)]
        return remote(ref, ref, dys.at[i], dyr.at[p, h], dev(to, c))

    def dy_wait(p, h):
        arrived(dxt.at[p, pl.ds(h * yhalf, yhalf)], dyr.at[p, h])

    dy_id = itertools.count()
    dy_list = [functools.partial(dy_own, 0, up, next(dy_id)), functools.partial(dy_own, 1, down, next(dy_id)),
               functools.partial(dy_own, 1, up, next(dy_id)), functools.partial(dy_own, 0, down, next(dy_id)),
               functools.partial(dy_fwd, down, 0, up, next(dy_id)), functools.partial(dy_fwd, up, 1, down, next(dy_id))]
    for m in dy_list:
        note(None, m)

    own_list[0]().start()
    own_list[1]().start()
    bx_start(0)
    own_list[2]().start()
    own_list[3]().start()
    dy_list[0]().start()
    dy_list[1]().start()

    def load_x(o, slot):
        return pltpu.make_async_copy(x_ref, dxv.at[slot], s_dxv.at[slot])

    load_x(0, 0).start()

    def own_b(b):
        return pltpu.make_async_copy(b_ref.at[pl.ds((2 * b + qc) * BLK, BLK)], sv.at[summed(b), pl.ds(0, BLK)], s_own.at[b])

    def own_b_out(b):
        return pltpu.make_async_copy(sv.at[summed(b), pl.ds(0, BLK)], bc.at[b, c], bxr.at[b, c])

    @pl.when(is_root)
    def _():
        for b in range(nb):
            own_b(b).start()

    order = tail + head
    ntot = len(order)

    def lin(n):
        b, q = block_of(n, order)
        src = l_ref.at[pl.ds(pl.multiple_of(q * ch, ch), ch), pl.ds(pl.multiple_of(b * BLK, BLK), BLK)]
        return pltpu.make_async_copy(src, lt_in.at[lax.rem(n, L_BUF)], s_lin.at[lax.rem(n, L_BUF)])

    def part_of(ref, i, full):
        n = cuts[i + 1] - cuts[i]
        return ref.at[pl.ds(cuts[i], n)] if full else ref.at[pl.ds(cuts[i], n), :, pl.ds(BLK, BLK)]

    def level(home, src_row, q, i):
        return jnp.where(src_row >= home, 2, 1) - q if i == 0 else jnp.int32(2)

    def by_level(i, lvl, fn):
        @pl.when(lvl == 2)
        def _():
            fn(True)

        if i == 0:
            @pl.when(lvl == 1)
            def _():
                fn(False)

    def ly(i, full):
        return remote(part_of(ltv, i, full), part_of(ltg.at[qc, r], i, full), lys.at[i], ltr.at[qc, r, i], dev(t, c))

    def ly_do(i, op):
        @pl.when(d != 0)
        def _():
            by_level(i, level(t, r, qc, i), lambda full: op(ly(i, full)))

    def l_own(i):
        return pltpu.make_async_copy(part_of(ltv, i, True), part_of(ltg.at[qc, r], i, True), ltr.at[qc, r, i])

    def l_zero(q, rr, j):
        src = lt_in.at[pl.ds(0, ndiag), pl.ds(0, BLK)]
        return pltpu.make_async_copy(src, ltg.at[q, rr, pl.ds(0, ndiag), :, pl.ds(j * BLK, BLK)], s_ltz.at[q, rr, j])

    def l_zeros(op):
        @pl.loop(0, nr)
        def _(rr):
            for q in range(2):
                lvl = level(r, rr, q, 0)
                mine = jnp.logical_and(is_root, jnp.logical_and(rr == r, qc == q))
                for j in range(2):
                    @pl.when(jnp.logical_and(lvl < 2 - j, jnp.logical_not(mine)))
                    def _():
                        op(l_zero(q, rr, j))

    for n in range(L_BUF - 1):
        lin(n).start()
    for b in range(1, NSUM):
        lth[pl.ds(b * BLK, BLK), pl.ds(0, b * ch)] = jnp.zeros((BLK, b * ch), BF)

    @pl.loop(0, ntot)
    def _(n):
        lin(n).wait()

        @pl.when(n + L_BUF - 1 < ntot)
        def _():
            lin(n + L_BUF - 1).start()

        blk = lt_in[lax.rem(n, L_BUF)].T

        @pl.when(n < nt)
        def _():
            ltv[n] = blk

        @pl.when(n >= nt)
        def _():
            b, q = block_of(n, order)
            lth[pl.ds(pl.multiple_of(b * BLK, BLK), BLK), pl.ds(pl.multiple_of(q * ch, ch), ch)] = blk

        for i in range(L_CUT):
            @pl.when(n == cuts[i + 1] - 1)
            def _():
                @pl.when(is_root)
                def _():
                    l_own(i).start()

                ly_do(i, lambda cp: cp.start())

    lt_in[...] = jnp.zeros_like(lt_in)
    l_zeros(lambda cp: cp.start())

    @pl.when(is_root)
    def _():
        for b in range(nb):
            own_b(b).wait()
        for b in range(nb):
            own_b_out(b).start()

    on_ring = par == lax.rem(r, 2)

    def l_do(q, e, w, to, op):
        rr = mod(r + lax.rem(e, nr), nr)

        def go(i, full):
            ref = part_of(ltg.at[q, rr], i, full)
            op(remote(ref, ref, lts.at[e, q, w], ltr.at[q, rr, i], dev(r, to)))

        for i in range(L_CUT):
            @pl.when(e // nr == i)
            def _():
                by_level(i, level(r, rr, q, i), functools.partial(go, i))

    def l_send(q, e, w, to):
        l_do(q, e, w, to, lambda cp: cp.start())

    def l_wait(q, e):
        rr = mod(r + lax.rem(e, nr), nr)
        mine = jnp.logical_and(is_root, jnp.logical_and(rr == r, qc == q))

        def go(i, full):
            arrived(part_of(ltg.at[q, rr], i, full), ltr.at[q, rr, i])

        for i in range(L_CUT):
            @pl.when(e // nr == i)
            def _():
                by_level(i, jnp.where(mine, 2, level(r, rr, q, i)), functools.partial(go, i))

    right = mod(c + 2, nc)
    left = mod(c - 2, nc)
    def l_fwd(q, e, op):
        side = lax.rem(e, nr) // 2
        from_left = c == mod(r + nr * q + 2, nc)

        @pl.when(from_left == (side == 0))
        def _():
            l_do(q, e, 0, jnp.where(from_left, right, left), op)

    def l_stage0(e):
        l_wait(qc, e)
        l_send(qc, e, 0, right)
        l_send(qc, e, 1, left)
        l_send(qc, e, 2, sib)

    def l_stage1(e):
        for q in range(2):
            l_wait(q, e)
            l_fwd(q, e, lambda cp: cp.start())
            l_send(q, e, 2, sib)

    def l_stage2(e):
        l_wait(1 - qc, e)
        l_send(1 - qc, e, 2, sib)

    def l_stage3(e):
        for q in range(2):
            l_wait(q, e)

    bh = BLK // B_CUT

    def b_ref_of(v, lo, hi):
        return bc.at[v // B_CUT, pl.ds(lo, hi - lo), pl.ds(lax.rem(v, B_CUT) * bh, bh)]

    def b_send(v, lo, hi, ss, rs, dd):
        ref = b_ref_of(v, lo, hi)
        return remote(ref, ref, bys.at[v, ss], byr.at[v, rs], dev(row_of(dd), c))

    def b_wait(v, lo, hi, rs):
        arrived(b_ref_of(v, lo, hi), byr.at[v, rs])

    ja = JA

    def by_share(v, fn):
        for k, jc in enumerate(JC):
            @pl.when(lax.rem(v, len(JC)) == k)
            def _():
                fn(jc)

    b_moves = [(0, lambda v, jc: b_send(v, 0, nc, 0, 0, 3)), (0, lambda v, jc: b_send(v, ja, nc, 1, 0, 1)),
               (3, lambda v, jc: b_send(v, 0, jc, 0, 0, 2)), (1, lambda v, jc: b_send(v, jc, nc, 0, 1, 2)),
               (2, lambda v, jc: b_send(v, 0, ja, 0, 1, 1))]

    mrow = SUM_UP
    prows = NSUM * BLK
    hrow = (prows - mrow) // SUM_CUT

    def sum_parts(o, i):
        if i is None:
            return pv.at[o, pl.ds(0, mrow)], prp.at[o], rbp, SUM_CUT
        return pv.at[o, pl.ds(pl.multiple_of(mrow + i * hrow, 16), hrow)], prm.at[o, i], rbm, i

    def sum_send(o, i):
        src, dst, _, k = sum_parts(o, i)
        to = row_of(mod(d + (1 if i is None else -1), nr))
        return remote(src, dst, prs.at[o, k], prr.at[o, k], dev(to, c))

    def sum_step(o, i):
        own, land, buf, k = sum_parts(o, i)
        arrived(land, prr.at[o, k])
        cp = pltpu.make_async_copy(land, buf, s_rb.at[0 if i is None else 1])
        cp.start()
        cp.wait()

        @pl.loop(0, buf.shape[0] // 16)
        def _(j):
            own[pl.ds(j * 16, 16)] = own[pl.ds(j * 16, 16)] + buf[pl.ds(j * 16, 16)]

        @pl.when(jnp.logical_not(is_root))
        def _():
            sum_send(o, i).start()

    def out_send(o, b, to):
        dst = db_ref.at[pl.ds((2 * b + qc) * BLK, BLK)]
        return remote(sv.at[o, pl.ds(b * BLK, BLK)], dst, dbs.at[o, b], dbr.at[2 * b + qc], dev(r, to))

    def out_local(o, b):
        dst = db_ref.at[pl.ds((2 * b + qc) * BLK, BLK)]
        return pltpu.make_async_copy(sv.at[o, pl.ds(b * BLK, BLK)], dst, dbr.at[2 * b + qc])

    def finish(o):
        @pl.loop(0, prows // 64)
        def _(i):
            sv[o, pl.ds(i * 64, 64)] = pv[o, pl.ds(i * 64, 64)].astype(BF)

        for b in range(NSUM):
            @pl.when(o == 0)
            def _():
                out_local(o, b).start()

            @pl.when(o != 0)
            def _():
                out_send(o, b, piece(o)).start()

    def partial(o):
        pv[o] = jnp.dot(lth[...], dxv[lax.rem(o, 2)], preferred_element_type=F32)

    offd = [next((n for n, x in enumerate(tail) if n >= ndiag and x[0] == b), nt) for b in range(NSUM, nb)]
    n2 = (nb - NSUM) * nr

    def t2_load(w, q, i):
        g, k = w // nr, lax.rem(w, 2)
        n = jnp.where(i == 0, g, table(g, offd) + i - 1)
        dst = ltb.at[k, pl.ds(q * BLK, BLK), pl.ds(pl.multiple_of(i * ch, ch), ch)]
        return pltpu.make_async_copy(ltg.at[q, lax.rem(w, nr), n], dst, s_ltb.at[k, q, i])

    def t2_loads(w, op):
        @pl.loop(0, nq - NSUM - w // nr)
        def _(i):
            for q in range(2):
                op(t2_load(w, q, i))

    def t2_start(w):
        t2_loads(w, lambda cp: cp.start())

    def t2_out(g):
        k = lax.rem(g, 2)
        return pltpu.make_async_copy(o2.at[k], db_ref.at[pl.ds((NSUM + g) * ch, ch)], s_o2.at[k])

    def t2_item(w):
        g, rr, k = w // nr, lax.rem(w, nr), lax.rem(w, 2)
        t2_loads(w, lambda cp: cp.wait())

        @pl.when(w + 1 < n2)
        def _():
            t2_start(w + 1)

        for gg in range(nb - NSUM):
            @pl.when(g == gg)
            def _():
                deep = (nq - NSUM - gg) * ch
                v = jnp.dot(ltb[k, :, pl.ds(0, deep)], dxtv[rr, pl.ds(gg * ch, deep)], preferred_element_type=F32)

                @pl.when(rr == 0)
                def _():
                    acc2[...] = v

                @pl.when(rr != 0)
                def _():
                    acc2[...] = acc2[...] + v

        @pl.when(rr == nr - 1)
        def _():
            @pl.when(g >= 2)
            def _():
                t2_out(g - 2).wait()
            o2[lax.rem(g, 2)] = acc2[...].astype(BF)
            t2_out(g).start()

    t3_order = [(b, q) for b in range(LATE) for q in range(b, nq)]
    n3 = len(t3_order)
    t3_last = [max(n for n, (bb, _) in enumerate(t3_order) if bb == b) for b in range(LATE)]

    def t3_load(n, o):
        b, q = block_of(n, t3_order)
        k = lax.rem(n, 2)
        rws = pl.ds(pl.multiple_of(q * ch, ch), ch)
        src = x_ref.at[rws] if o == 0 else dxg.at[mod(c + o, nc), rws]
        return pltpu.make_async_copy(src, dt.at[k, :, pl.ds(pl.multiple_of(mod(c + o, nc) * width, width), width)], s_dt.at[k, o])

    def bv_load(b, j):
        k = lax.rem(b, 2)
        return pltpu.make_async_copy(bc.at[b, j], bv.at[k, :, pl.ds(j * width, width)], s_bv.at[k, j])

    def t3_out(n):
        k = lax.rem(n, 2)
        return pltpu.make_async_copy(o3.at[k], dl_ref.at[n], s_o3.at[k])

    def t3_item(n):
        b, q = block_of(n, t3_order)
        k = lax.rem(n, 2)
        for o in range(nc):
            t3_load(n, o).wait()

        @pl.when(n + 1 < n3)
        def _():
            for o in range(nc):
                t3_load(n + 1, o).start()

        @pl.when(q == b)
        def _():
            for j in range(nc):
                bv_load(b, j).wait()

        acc3[...] = lax.dot_general(dt[k], bv[lax.rem(b, 2)], (((1,), (1,)), ((), ())), preferred_element_type=F32)

        @pl.when(n >= 2)
        def _():
            t3_out(n - 2).wait()

        _round_lower(acc3, o3.at[k], b, q, (r, nr), (c, nc))
        t3_out(n).start()
    b_ready = [max(x[B_CUT * b + B_CUT - 1] for x in b_slot) for b in range(nb)]
    l_ready = [max(x[nr * i + nr - 1] for x in l_slot) for i in range(L_CUT)]
    t2_need = [l_ready[min(w // nr + 1, L_CUT - 1)] for w in range(n2)]

    def packed(start, ready):
        out = []
        for n in range(len(ready)):
            out.append(max(start, ready[n], out[-1] + 1 if out else 0))
        return out

    t2_slots = packed(T2_A, t2_need[1:] + t2_need[-1:])
    t3_slots, bv_slots = [], []
    for b in range(LATE):
        bv_slots.append(max(b_ready[b], T3_A - 1 if b < 2 else t3_slots[t3_last[b - 2]]))
        t3_slots = packed(T3_A, t3_slots + [bv_slots[b] + 1] * (nq - b))
    assert T2_A > max(l_ready[1], Y_EVENTS[6]) and Y_EVENTS[6] > max(Y_EVENTS[3:6])
    assert T3_A > max(load_x_at[-1], DX_EVENTS[-1])
    lists = (sum_at, b_slot, l_slot)
    assert all(a < b for f in lists + ((SUM_X,),) for x in f for a, b in zip(x[:-1], x[1:]))
    assert all(sum_at[0][u * SUM_CUT] > SUM_X[summed(u)] for u in range(nc))
    assert all(a < b for f in lists for y, z in zip(f[:-1], f[1:]) for a, b in zip(y, z))
    assert all(SUM_X[o - 2] < load_x_at[o] for o in range(2, nc))
    assert all(max(DX_EVENTS[o:o + 2]) <= load_x_at[o + 2] for o in (0, 2, 4))
    assert all(b_slot[0][B_CUT * b] <= sum_at[-1][b * SUM_CUT + SUM_CUT - 1] for b in range(nb))
    slots = 1 + max(t3_slots[-1], t2_slots[-1], sum_at[-1][-1], b_ready[-1], l_ready[-1])

    down_depth = nr - 1 - d
    up_depth = mod(d - 1, nr)
    off_ring = jnp.logical_not(on_ring)

    def listed(vals):
        return lambda n: table(n, tuple(vals) + (slots,))

    events = []

    def event(slot, fn):
        events.append((slot, fn))

    def dx_event(i):
        p, h, ms = ev[i]
        dx_wait(p, h)
        for m in ms:
            m().start()

    def dx_rest():
        for m in own_list[4:]:
            m().start()

    def bx_event(b):
        bx_start(b)

    def y_first():
        dy_list[2]().start()
        dy_list[3]().start()

    def y_event(i):
        if i == 1:
            dy_wait(down, 0)
            dy_list[4]().start()
        elif i == 2:
            dy_wait(up, 1)
            dy_list[5]().start()
        elif i == 3:
            dy_wait(down, 1)
        elif i == 4:
            dy_wait(up, 0)
        else:
            dy_wait(opp, 0)
            dy_wait(opp, 1)

    def y_load(op):
        for i in range(nr):
            rr = mod(r + i, nr)
            src = x_ref.at[pl.ds(yrow0, 2 * yhalf)] if i == 0 else dxt.at[rr]
            op(pltpu.make_async_copy(src, dxtv.at[rr], s_dxt.at[i]))

    def t2_first():
        l_zeros(lambda cp: cp.wait())
        t2_start(0)
        y_load(lambda cp: cp.wait())

    def t3_first():
        for o in range(nc):
            t3_load(0, o).start()

    def bv_event(b):
        for j in range(nc):
            bv_load(b, j).start()

    for i in range(len(ev)):
        event(DX_EVENTS[i], functools.partial(dx_event, i))
    event(DX_SEND, dx_rest)
    for b in range(1, nb):
        event(bx_at[b], functools.partial(bx_event, b))
    event(Y_EVENTS[0], y_first)
    for i in range(1, 6):
        event(Y_EVENTS[i], functools.partial(y_event, i))
    event(Y_EVENTS[6], lambda: y_load(lambda cp: cp.start()))
    n_first = len(events)
    event(T2_A - 1, t2_first)
    event(T3_A - 1, t3_first)
    for b in range(LATE):
        event(bv_slots[b], functools.partial(bv_event, b))

    def event_flow(lo, hi):
        part = sorted(range(lo, hi), key=lambda i: events[i][0])
        at = sorted({events[i][0] for i in part})
        masks = [sum(1 << (i - lo) for i in part if events[i][0] == x) for x in at]

        def run(k):
            mask = table(k, masks)
            for i in range(lo, hi):
                @pl.when(jnp.bitwise_and(mask, 1 << (i - lo)) != 0)
                def _():
                    events[i][1]()

        return listed(at), len(at), run

    def b_due(v):
        @pl.when(is_root)
        def _():
            @pl.when(lax.rem(v, B_CUT) == 0)
            def _():
                @pl.loop(0, nc)
                def _(j):
                    arrived(bc.at[v // B_CUT, j], bxr.at[v // B_CUT, j])
            b_moves[0][1](v, nc).start()
            b_moves[1][1](v, nc).start()

        @pl.when(d == 3)
        def _():
            b_wait(v, 0, nc, 0)
            by_share(v, lambda jc: b_moves[2][1](v, jc).start())

        @pl.when(d == 1)
        def _():
            b_wait(v, ja, nc, 0)
            by_share(v, lambda jc: b_moves[3][1](v, jc).start())

        @pl.when(d == 2)
        def _():
            by_share(v, lambda jc: b_wait(v, 0, jc, 0))
            b_moves[4][1](v, nc).start()
            by_share(v, lambda jc: b_wait(v, jc, nc, 1))

    def b_last(v):
        b_wait(v, 0, ja, 1)

    def l_due(e):
        @pl.when(is_root)
        def _():
            l_stage0(e)

        @pl.when(off_ring)
        def _():
            l_stage3(e)

        @pl.when(jnp.logical_and(on_ring, jnp.logical_not(is_root)))
        def _():
            l_stage1(e)

    def sum_due(o, i, depth):
        @pl.when(depth == 0)
        def _():
            sum_send(o, i).start()

        @pl.when(depth > 0)
        def _():
            sum_step(o, i)

    def down_due(n):
        sum_due(summed(n // SUM_CUT), lax.rem(n, SUM_CUT), down_depth)

    def load_due(o):
        p = piece(o)
        k = lax.rem(o, 2)

        @pl.when(k == 1)
        def _():
            dx_wait(p, 0)
            dx_wait(p, 1)

        @pl.when(o > 0)
        def _():
            pltpu.make_async_copy(dxg.at[p], dxv.at[k], s_dxv.at[k]).start()

    def part_due(o):
        load_x(0, lax.rem(o, 2)).wait()
        partial(o)

    def stage(lines, k, total):
        first = jnp.int32(slots)
        num = jnp.int32(0)
        for i, (f, m, _) in enumerate(lines):
            first = jnp.where(k == i, f, first)
            num = jnp.where(k == i, m, num)
        return lambda n: jnp.where(n < total, first + n * num // 4, slots)

    def up_due(u):
        sum_due(summed(u), None, up_depth)

        @pl.when(is_root)
        def _():
            finish(summed(u))

    none = jnp.int32(-1)
    flows = [event_flow(0, n_first)[::2],
             (stage(L_LINES, jnp.where(is_root, 0, jnp.where(off_ring, 3, 1)), ne), l_due),
             (stage(L_LINES, jnp.where(is_root, 2, none), ne), l_stage2),
             (stage(B_LINES, jnp.where(d == 0, 0, jnp.where(d == 2, 2, 1)), nv), b_due),
             (stage(B_LINES, jnp.where(d == 1, 3, none), nv), b_last),
             (stage(SUM_LINES, down_depth, nc * SUM_CUT), down_due),
             (lambda n: stage(SUM_LINES, up_depth, nc * SUM_CUT)(n * SUM_CUT + SUM_CUT - 1), up_due),
             (listed(load_x_at), load_due),
             (listed(SUM_X), part_due),
             event_flow(n_first, n_first + 2)[::2],
             (listed(t2_slots), t2_item), (listed(t3_slots), t3_item), event_flow(n_first + 2, len(events))[::2]]

    def slot(s, carry):
        nxt = []
        for (when, fn), (n, at) in zip(flows, carry):
            def go(n, fn=fn, when=when):
                fn(n)
                return n + 1, when(n + 1)

            def stay(n, at=at):
                return n, at

            nxt.append(lax.cond(at == s, go, stay, n))
        return tuple(nxt)

    lax.fori_loop(0, slots, slot, tuple((jnp.int32(0), jnp.int32(when(jnp.int32(0)))) for when, _ in flows))

    for g in (n2 // nr - 2, n2 // nr - 1):
        t2_out(g).wait()
    for n in (n3 - 2, n3 - 1):
        t3_out(n).wait()
    for i in range(2 * NSUM):
        arrived(db_ref.at[pl.ds(i * BLK, BLK)], dbr.at[i])

    for cond, make, _ in sends:
        if cond is None:
            make().wait_send()
        else:
            @pl.when(cond)
            def _():
                make().wait_send()

    @pl.loop(0, nv)
    def _(v):
        for dd, make in b_moves:
            @pl.when(d == dd)
            def _():
                by_share(v, lambda jc: make(v, jc).wait_send())

    def sent(cp):
        cp.wait_send()

    for i in range(L_CUT):
        ly_do(i, sent)

    @pl.loop(0, ne)
    def _(e):
        @pl.when(is_root)
        def _():
            l_do(qc, e, 0, right, sent)
            l_do(qc, e, 1, left, sent)
            l_do(qc, e, 2, sib, sent)
            l_do(1 - qc, e, 2, sib, sent)

        @pl.when(jnp.logical_and(on_ring, jnp.logical_not(is_root)))
        def _():
            for q in range(2):
                l_fwd(q, e, sent)
                l_do(q, e, 2, sib, sent)

    @pl.loop(0, 8)
    def _(o):
        @pl.when(jnp.logical_not(is_root))
        def _():
            for i in (None,) + tuple(range(SUM_CUT)):
                sum_send(o, i).wait_send()

        @pl.when(jnp.logical_and(is_root, o != 0))
        def _():
            for b in range(NSUM):
                out_send(o, b, piece(o)).wait_send()


def solution(mesh):
    nr = mesh.shape["row"]
    nc = mesh.shape["col"]
    spec = P(("batch", "row"), "col")

    def per_device(lower_tri, right_side, grad_out):
        rows, cols = lower_tri.shape
        width = right_side.shape[1]
        ch = 2 * BLK
        nq, nb = rows // ch, cols // BLK
        nt = sum(nq - b for b in range(NSUM, nb))
        ntot = sum(nq - b for b in range(nb))
        yrows = rows - NSUM * ch
        sd = jax.ShapeDtypeStruct
        n_early = sum(nq - b for b in range(LATE))
        n_late = sum(nq - b for b in range(LATE, nb))
        outs = (sd((rows, width), BF), sd((n_early, ch, BLK), BF), sd((nc, rows, width), BF), sd((nb, nc, BLK, width), BF),
                sd((nr, yrows, width), BF), sd((2, nr, nt, BLK, ch), BF),
                sd((nc, SUM_CUT, (NSUM * BLK - SUM_UP) // SUM_CUT, width), F32), sd((nc, SUM_UP, width), F32))
        vm = pltpu.VMEM
        dma = pltpu.SemaphoreType.DMA
        scratch = [vm((L_BUF, ch, BLK), BF), vm((nt, BLK, ch), BF), vm((NSUM * BLK, rows), BF), vm((2, rows, width), BF), vm((nc, NSUM * BLK, width), F32),
                   vm(((NSUM * BLK - SUM_UP) // SUM_CUT, width), F32), vm((SUM_UP, width), F32), vm((nc, NSUM * BLK, width), BF),
                   vm((nr, yrows, width), BF), vm((2, ch, (nq - NSUM) * ch), BF), vm((ch, width), F32), vm((2, ch, width), BF),
                   vm((2, ch, nc * width), BF), vm((2, BLK, nc * width), BF), vm((ch, BLK), F32), vm((2, ch, BLK), BF),
                   dma((14,)), dma((nc, 2)), dma((nb, 2)), dma((nb, nc)), dma((nb * B_CUT, 2)), dma((nb * B_CUT, 2)),
                   dma((6,)), dma((nr, 2)), dma((L_CUT,)), dma((nr * L_CUT, 2, 3)), dma((2, nr, L_CUT)),
                   dma((nc, SUM_CUT + 1)), dma((nc, SUM_CUT + 1)), dma((nc, NSUM)), dma((2 * NSUM,)),
                   dma((2, nr, 2)), dma((L_BUF,)), dma((2,)), dma((2,)), dma((nr,)), dma((2, 2, nq - NSUM)), dma((2,)), dma((2, nc)), dma((2, nc)),
                   dma((2,)), dma((nb,))]
        res = pl.pallas_call(
            functools.partial(_kernel, nr, nc),
            out_shape=outs,
            in_specs=[pl.BlockSpec(memory_space=pl.ANY)] * 3,
            out_specs=tuple(pl.BlockSpec(memory_space=pl.ANY) for _ in outs),
            scratch_shapes=scratch,
            compiler_params=pltpu.CompilerParams(collective_id=0, has_side_effects=True, vmem_limit_bytes=VMEM_BYTES),
            name="tri_backward",
        )(lower_tri, right_side, grad_out)
        db, tiles, dxg, bc = res[:4]
        far = nq - LATE
        return pl.pallas_call(
            functools.partial(_last_kernel, nr, nc),
            out_shape=(sd((rows, width), BF), sd((rows, cols), BF)),
            in_specs=[pl.BlockSpec(memory_space=pl.ANY)] * 5,
            out_specs=(pl.BlockSpec(memory_space=pl.ANY),) * 2,
            scratch_shapes=[vm((far, ch, nc * width), BF), vm((far, BLK, nc * width), BF), vm((n_early, ch, BLK), BF), vm((rows, width), BF),
                            vm((ch, BLK), F32), vm((n_late, ch, BLK), BF), vm((ch, BLK), BF),
                            dma((far, nc)), dma((far, nc)), dma((n_early,)), dma((n_early,)), dma((n_late,)),
                            dma((nb * (nb - 1) // 2,)), dma((2,))],
            compiler_params=pltpu.CompilerParams(vmem_limit_bytes=VMEM_BYTES),
            name="tri_backward_last",
        )(grad_out, dxg, bc, tiles, db)

    return jax.shard_map(per_device, mesh=mesh, in_specs=(spec, spec, spec), out_specs=(spec, spec), check_vma=False)
```
